128 devices in a mesh: row: 16 (over z, x), col: 8 (over y, core).
Axes of the slice: x: 4, y: 4, z: 4, core: 2. Of those that a mesh axis runs over, the one named last changes fastest.
Arguments:
- amplitudes: float32 [192, 10, 10, 2048], P('row', None, None, 'col'), may hold values from -6 to 6
- old_blocks: int32 [16, 12], replicated, may hold values from 0 to 135, as said below
- old_counts: int32 [16], replicated, may hold values from 1 to 12, as said below
- new_phase: int32 [1], replicated, may hold values from 0 to 15
- fock: float32 [160, 160], P('row'), may hold values from -0.5 to 0.5
Outputs:
- contracted: float32 [16, 10, 160, 2048], P('row', None, None, 'col')
The draws below stay inside these ranges and needn't reach their ends.
Inputs may be any that keep to these rules, and one draw needn't show every extreme that they name: `old_blocks`: over the live slots of all row devices every tile pair id 0 to 135 stands exactly once; ids in slots that are not live are arbitrary. For every residue r mod 16, at most 3 live blocks of one row device hold a tile whose index is r mod 16, and some device reaches 3 for some r. `old_counts`: the counts sum to 136; some device has exactly 12.
All inputs are finite; a program needn't handle non-finite values.
Results may differ from the reference program's by a relative error of at most 0.00007.
Values sent between devices are 32-bit elements; how exact they have to be, the bound alone decides.
A program may use at most 128 MiB of HBM per device.

```python
import jax
import jax.numpy as jnp
import numpy as np
from jax import lax

V = 160
NT = 16
BT = 10
OPAIRS = 2048
SLOTS = 12
N_ROW = 16


def tile_lists():
    count = NT * (NT + 1) // 2
    first_tile = np.zeros((count,), np.int32)
    second_tile = np.zeros((count,), np.int32)
    for low in range(NT):
        for high in range(low, NT):
            ident = low * NT - low * (low - 1) // 2 + (high - low)
            first_tile[ident] = low
            second_tile[ident] = high
    return (first_tile, second_tile)


def layout_tables(key):
    inner = jax.random.fold_in(key, 7)
    key_full, key_extra, key_res, key_odd, key_rest, key_noise, key_junk = jax.random.split(inner, 7)
    nblocks = NT * (NT + 1) // 2
    first_np, second_np = tile_lists()
    first_tile = jnp.asarray(first_np)
    second_tile = jnp.asarray(second_np)
    residue = jax.random.randint(key_res, (), 0, N_ROW)
    owned = ((first_tile % N_ROW == residue) | (second_tile % N_ROW == residue)).astype(jnp.int32)
    klass = (first_tile + second_tile) % NT
    odd_order = 2 * jax.random.permutation(key_odd, NT // 2).astype(jnp.int32) + 1
    evens = 2 * jnp.arange(NT // 2, dtype=jnp.int32)
    leftover = jax.random.permutation(key_rest, jnp.concatenate([odd_order[4:], evens])).astype(jnp.int32)
    order = jnp.concatenate([odd_order[:4], leftover]).astype(jnp.int32)
    rank = jnp.zeros((NT,), jnp.int32).at[order].set(jnp.arange(NT, dtype=jnp.int32))
    block_rank = rank[klass]
    noise = jax.random.permutation(key_noise, nblocks).astype(jnp.int32)
    group = jnp.where((block_rank == 0) & (owned == 1), 0, jnp.where(block_rank == 0, 100, block_rank))
    sort_key = group * 1000 + (1 - owned) * 200 + noise
    sequence = jnp.argsort(sort_key, stable=True).astype(jnp.int32)
    full = jax.random.randint(key_full, (), 0, N_ROW)
    rest = nblocks - SLOTS
    base = rest // (N_ROW - 1)
    extra = rest - base * (N_ROW - 1)
    shuffle = jax.random.permutation(key_extra, N_ROW - 1)
    others = base + (shuffle < extra).astype(jnp.int32)
    pos_counts = jnp.concatenate([jnp.full((1,), SLOTS, jnp.int32), others.astype(jnp.int32)])
    pos_starts = jnp.cumsum(pos_counts) - pos_counts
    device = jnp.arange(N_ROW, dtype=jnp.int32)
    place = (device - full) % N_ROW
    counts = pos_counts[place].astype(jnp.int32)
    starts = pos_starts[place]
    slot = jnp.arange(SLOTS, dtype=jnp.int32)[None, :]
    where_at = jnp.clip(starts[:, None] + slot, 0, nblocks - 1)
    junk = jax.random.randint(key_junk, (N_ROW, SLOTS), 0, nblocks)
    blocks = jnp.where(slot < counts[:, None], sequence[where_at], junk).astype(jnp.int32)
    return (blocks, counts)


def draw_old_blocks(key, part):
    return layout_tables(key)[0]


def draw_old_counts(key, part):
    return layout_tables(key)[1]


def block_levels(stream_key, extent, cuts, smallest, high):
    def one(dim, parts):
        draws = jax.random.uniform(jax.random.fold_in(jax.random.fold_in(stream_key, 6), dim), (parts,), jnp.float32, smallest / len(cuts), high / len(cuts))
        return jnp.repeat(jnp.exp(draws), extent[dim] // parts).reshape((-1,) + (1,) * (len(extent) - dim - 1))

    factor_of = one(*cuts[0])
    for cut in cuts[1:]:
        factor_of = factor_of * one(*cut)
    return factor_of


def normal_values(rng, shape, deviation, most, cuts=(), kind=jnp.bfloat16):
    gain = block_levels(rng, shape, cuts, -0.22, 0.18) if cuts else 1.0
    drawn = jax.random.normal(rng, shape, jnp.float32) * deviation * gain
    return jnp.minimum(jnp.maximum(drawn, -most), most).astype(kind)


def setup_inputs(seed: int = 0) -> dict:
    seeds = jax.random.split(jax.random.key(seed), 6)
    return {
        "amplitudes": normal_values(seeds[0], (N_ROW * SLOTS, BT, BT, OPAIRS), 1.0, 6.0, ((0, 16), (3, 8)), jnp.float32),
        "old_blocks": draw_old_blocks(jax.random.fold_in(seeds[5], 71), 0),
        "old_counts": draw_old_counts(jax.random.fold_in(seeds[5], 71), 0),
        "new_phase": jax.random.randint(seeds[3], (1,), 0, N_ROW).astype(jnp.int32),
        "fock": normal_values(seeds[4], (V, V), V ** -0.5, 0.5, ((0, 16),), jnp.float32),
    }


def pair_table():
    table = np.zeros((NT, NT), np.int32)
    for first in range(NT):
        for second in range(NT):
            low = min(first, second)
            high = max(first, second)
            table[first, second] = low * NT - low * (low - 1) // 2 + (high - low)
    return table


def reference(amplitudes, old_blocks, old_counts, new_phase, fock):
    nblocks = NT * (NT + 1) // 2
    live = jnp.arange(SLOTS, dtype=jnp.int32)[None, :] < old_counts[:, None]
    target = jnp.where(live, old_blocks, nblocks).reshape(-1).astype(jnp.int32)
    blocks = jnp.zeros((nblocks, BT, BT, amplitudes.shape[3]), jnp.float32)
    blocks = blocks.at[target].set(amplitudes, mode="drop")
    table = jnp.asarray(pair_table())
    upper = blocks[table.reshape(-1)].reshape(NT, NT, BT, BT, -1)
    upper = jnp.transpose(upper, (0, 2, 1, 3, 4)).reshape(V, V, -1)
    index = jnp.arange(V, dtype=jnp.int32)
    lower_mask = (index[:, None] < index[None, :])[:, :, None]
    upper_mask = (index[:, None] > index[None, :])[:, :, None]
    dense = jnp.where(lower_mask, upper, jnp.where(upper_mask, -jnp.swapaxes(upper, 0, 1), 0.0))
    half = jnp.einsum("ac,cbj->baj", fock, dense, precision=lax.Precision.HIGHEST)
    per_dev = NT // N_ROW
    position = jnp.arange(NT, dtype=jnp.int32)
    owner = position // per_dev
    within = position % per_dev
    tiles = (owner - new_phase[0]) % N_ROW + within * N_ROW
    return half.reshape(NT, BT, V, -1)[tiles.astype(jnp.int32)]
```

```python
import jax
import jax.numpy as jnp
import numpy as np
from jax import lax
from jax.experimental import pallas as pl
from jax.experimental.pallas import tpu as pltpu
from jax.sharding import PartitionSpec as P

NT = 16
BT = 10
NR = 16
SLOTS = 12
PIECE = 13
SROWS = 160
CROWS = NT * PIECE
LANES = 128
TYPE_A = 10
MESH = pl.DeviceIdType.MESH


def piece_tables():
    pairs = [(x, y, h) for h in range(2) for x in range(BT) for y in range(x + 1, BT)]
    diagonal = [(x, x, h) for h in range(2) for x in range(BT)]
    pieces = []
    for m in range(NR):
        rows = []
        for _ in range(6 if m < TYPE_A else 5):
            x, y, h = pairs.pop(0)
            rows += [(x, y, h), (y, x, h)]
        for _ in range(1 if m < TYPE_A else 2):
            if diagonal:
                rows.append(diagonal.pop(0))
        pieces.append(rows)
    assert not pairs and not diagonal
    where = {row: (m, j) for m, rows in enumerate(pieces) for j, row in enumerate(rows)}
    return pieces, where


def kernel(
    table_ref, amp_hbm, fock_ref, out_hbm,
    amp, send1, recv1, send2, recv2, coef_a, coef_b, fgather, ffull, dense, outv,
    in_sem, s1_sem, r1_sem, s2_sem, r2_sem, fs_sem, fr_sem, o_sem,
):
    pieces, where = piece_tables()
    me = lax.axis_index("row")
    barrier = pltpu.get_barrier_semaphore()
    load = pltpu.make_async_copy(amp_hbm, amp, in_sem)
    load.start()
    for d in range(1, NR):
        pl.semaphore_signal(barrier, inc=1, device_id={"row": (me + d) % NR}, device_id_type=MESH)
    load.wait()

    @pl.loop(0, SLOTS)
    def _(slot):
        for m in range(NR):
            for j, (x, y, h) in enumerate(pieces[m]):
                send1[m, pl.ds(slot * PIECE + j, 1), :] = amp[slot, x, pl.ds(y, 1), pl.ds(h * LANES, LANES)]

    pl.semaphore_wait(barrier, NR - 1)

    def phase1(d):
        to = (me + d) % NR
        return pltpu.make_async_remote_copy(
            src_ref=send1.at[to], dst_ref=recv1.at[me, pl.ds(8, SROWS)], send_sem=s1_sem.at[to], recv_sem=r1_sem.at[me],
            device_id={"row": to}, device_id_type=MESH)

    def fock_copy(d):
        to = (me + d) % NR
        return pltpu.make_async_remote_copy(
            src_ref=fock_ref, dst_ref=fgather.at[me], send_sem=fs_sem.at[to], recv_sem=fr_sem.at[me],
            device_id={"row": to}, device_id_type=MESH)

    def phase2(d):
        to = (me + d) % NR
        return pltpu.make_async_remote_copy(
            src_ref=send2.at[to], dst_ref=recv2.at[me], send_sem=s2_sem.at[to], recv_sem=r2_sem.at[me],
            device_id={"row": to}, device_id_type=MESH)

    @pl.loop(1, NR)
    def _(d):
        phase1(d).start()

    @pl.loop(1, NR)
    def _(d):
        fock_copy(d).start()

    recv1[me, pl.ds(8, SROWS), :] = send1[me]
    fgather[me] = fock_ref[...]
    row = lax.broadcasted_iota(jnp.int32, (16, LANES), 0)
    is_pair = (row < 10) | ((row < 12) & (me < TYPE_A))
    odd = row % 2 == 1
    one = jnp.ones((16, LANES), jnp.float32)
    zero = jnp.zeros((16, LANES), jnp.float32)
    coef_a[0] = one
    coef_b[0] = zero
    coef_a[1] = jnp.where(is_pair, 0.0, -one)
    coef_b[1] = jnp.where(is_pair, -one, 0.0)
    coef_a[2] = jnp.where(is_pair & ~odd, one, 0.0)
    coef_b[2] = jnp.where(is_pair & odd, -one, 0.0)
    up_mask = ((row % 2 == 0) & (row < 12))[:PIECE]

    @pl.loop(1, NR)
    def _(d):
        src = (me + d) % NR
        pltpu.make_async_remote_copy(
            src_ref=send1.at[src], dst_ref=recv1.at[src, pl.ds(8, SROWS)], send_sem=s1_sem.at[src], recv_sem=r1_sem.at[src],
            device_id={"row": src}, device_id_type=MESH).wait_recv()

    def pack2(to, dst):
        for c in range(NT):
            code = table_ref[to, c]
            at = code // 4
            kind = code % 4
            s = at // SROWS
            r = at % SROWS
            v = recv1[s, pl.ds(r + 8, PIECE), :]
            swapped = jnp.where(up_mask, recv1[s, pl.ds(r + 9, PIECE), :], recv1[s, pl.ds(r + 7, PIECE), :])
            dst[to if dst is send2 else me, pl.ds(c * PIECE, PIECE), :] = (
                coef_a[kind, :PIECE] * v + coef_b[kind, :PIECE] * swapped)

    @pl.loop(1, NR)
    def _(d):
        pack2((me + d) % NR, send2)
        phase2(d).start()

    pack2(me, recv2)

    @pl.loop(1, NR)
    def _(d):
        src = (me + d) % NR
        pltpu.make_async_remote_copy(
            src_ref=fock_ref, dst_ref=fgather.at[src], send_sem=fs_sem.at[src], recv_sem=fr_sem.at[src],
            device_id={"row": src}, device_id_type=MESH).wait_recv()

    for d in range(NR):
        ffull[pl.ds(d * BT, BT), :] = fgather[d]

    @pl.loop(1, NR)
    def _(d):
        src = (me + d) % NR
        pltpu.make_async_remote_copy(
            src_ref=send2.at[src], dst_ref=recv2.at[src], send_sem=s2_sem.at[src], recv_sem=r2_sem.at[src],
            device_id={"row": src}, device_id_type=MESH).wait_recv()

    f = ffull[...]
    for y in range(BT):
        for h in range(2):
            for x in range(BT):
                m, j = where[(x, y, h)]
                dense[h, y, pl.ds(x, NT, stride=BT), :] = recv2[m, pl.ds(j, NT, stride=PIECE), :]
    for y in range(BT):
        column = jnp.concatenate([dense[0, y], dense[1, y]], axis=1)
        outv[y] = jnp.dot(f, column, precision=lax.Precision.HIGHEST, preferred_element_type=jnp.float32)
        pltpu.make_async_copy(outv.at[y], out_hbm.at[0, y], o_sem.at[y]).start()

    @pl.loop(1, NR)
    def _(d):
        phase1(d).wait_send()
        fock_copy(d).wait_send()
        phase2(d).wait_send()

    for y in range(BT):
        pltpu.make_async_copy(outv.at[y], out_hbm.at[0, y], o_sem.at[y]).wait()


def body(amplitudes, old_blocks, old_counts, new_phase, fock):
    e = lax.broadcasted_iota(jnp.int32, (NR, NT, NR * SLOTS), 0)
    c = lax.broadcasted_iota(jnp.int32, (NR, NT, NR * SLOTS), 1)
    live = (jnp.arange(SLOTS, dtype=jnp.int32)[None, :] < old_counts[:, None])
    ids = jnp.where(live, old_blocks, -1).reshape(1, 1, -1)
    b = (e - new_phase[0] + NR) % NR
    low = jnp.minimum(b, c)
    high = jnp.maximum(b, c)
    ident = low * NT - low * (low - 1) // 2 + (high - low)
    where_at = np.arange(NR)[:, None] * SROWS + np.arange(SLOTS)[None, :] * PIECE
    at = jnp.sum(jnp.where(ids == ident, jnp.asarray(where_at.reshape(1, 1, -1), jnp.int32), 0), axis=2)
    b2 = b[:, :, 0]
    c2 = c[:, :, 0]
    kind = jnp.where(c2 < b2, 0, jnp.where(c2 > b2, 1, 2))
    table = at * 4 + kind
    nocc = amplitudes.shape[3]
    return pl.pallas_call(
        kernel,
        name="fock_two_phase",
        out_shape=jax.ShapeDtypeStruct((1, BT, NT * BT, nocc), jnp.float32),
        in_specs=[
            pl.BlockSpec(memory_space=pltpu.SMEM),
            pl.BlockSpec(memory_space=pl.ANY),
            pl.BlockSpec(memory_space=pltpu.VMEM),
        ],
        out_specs=pl.BlockSpec(memory_space=pl.ANY),
        scratch_shapes=[
            pltpu.VMEM(amplitudes.shape, jnp.float32),
            pltpu.VMEM((NR, SROWS, LANES), jnp.float32),
            pltpu.VMEM((NR, 8 + SROWS + 8, LANES), jnp.float32),
            pltpu.VMEM((NR, CROWS, LANES), jnp.float32),
            pltpu.VMEM((NR, CROWS, LANES), jnp.float32),
            pltpu.VMEM((3, 16, LANES), jnp.float32),
            pltpu.VMEM((3, 16, LANES), jnp.float32),
            pltpu.VMEM((NR, BT, NT * BT), jnp.float32),
            pltpu.VMEM((NT * BT, NT * BT), jnp.float32),
            pltpu.VMEM((2, BT, NT * BT, LANES), jnp.float32),
            pltpu.VMEM((BT, NT * BT, nocc), jnp.float32),
            pltpu.SemaphoreType.DMA,
            pltpu.SemaphoreType.DMA((NR,)),
            pltpu.SemaphoreType.DMA((NR,)),
            pltpu.SemaphoreType.DMA((NR,)),
            pltpu.SemaphoreType.DMA((NR,)),
            pltpu.SemaphoreType.DMA((NR,)),
            pltpu.SemaphoreType.DMA((NR,)),
            pltpu.SemaphoreType.DMA((BT,)),
        ],
        compiler_params=pltpu.CompilerParams(
            collective_id=0, has_side_effects=True, vmem_limit_bytes=48 << 20),
    )(table, amplitudes, fock)


def solution(mesh):
    return jax.shard_map(
        body,
        mesh=mesh,
        in_specs=(P("row", None, None, "col"), P(), P(), P(), P("row", None)),
        out_specs=P("row", None, None, "col"),
        check_vma=False,
    )
```

```python
import jax
import jax.numpy as jnp
from jax import lax
from jax.experimental import pallas as pl
from jax.experimental.pallas import tpu as pltpu
from jax.sharding import PartitionSpec as P

NT = 16
BT = 10
NR = 16
SLOTS = 12
LANES = 128
SPLIT = 8
MESH = pl.DeviceIdType.MESH
S1 = 160
R1 = 128
FRONT = 16
P2 = 208
LATE = 128
OTHERS = NT - 1
HEAD = (SPLIT // 2, 2)
ROWS1 = SPLIT * SLOTS
ROWS2 = SPLIT * OTHERS + HEAD[0]


def is_long(m):
    return (m // 4 + m) % 2 == 0


def late_rows1(long):
    return (5 if long else 4) * SLOTS


def late_rows2(long):
    return (5 if long else 4) * OTHERS + HEAD[1]


def piece_tables():
    pairs = [(x, y, h) for h in range(2) for x in range(BT) for y in range(x + 1, BT)]
    diagonal = [(x, x, h) for h in range(2) for x in range(BT)]
    pieces = []
    for m in range(NR):
        rows = []
        for _ in range(6 if is_long(m) or m in (1, 14) else 5):
            x, y, h = pairs.pop(0)
            rows += [(x, y, h), (y, x, h)]
        while len(rows) < (13 if is_long(m) else 12):
            rows.append(diagonal.pop(0))
        pieces.append(rows)
    assert not pairs and not diagonal
    return pieces


def remote(src, dst, send, recv, to):
    return pltpu.make_async_remote_copy(
        src_ref=src, dst_ref=dst, send_sem=send, recv_sem=recv, device_id=to, device_id_type=MESH)


def wait_rows(ref, rows, sem):
    part = ref.at[pl.ds(0, rows)]
    pltpu.make_async_copy(part, part, sem).wait()


def kernel(
    phase_ref, blocks_hbm, counts_hbm, amp_hbm, fock_hbm, out_ref,
    blocks_ref, counts_ref, fock_ref, amp, send1, first1, second1, send2, recv2, coef_a, coef_b,
    ftiles, fgather, ffull, turned_high, turned_low, dense, vtable, table,
    a_sem, b_sem, c_sem, f_sem, t_sem, s1_sem, r1_sem, s2_sem, r2_sem, fs_sem, fr_sem, ds_sem, dr_sem,
):
    pieces = piece_tables()
    me = lax.axis_index("row")
    col = lax.axis_index("col")
    core = col % 2
    partner = col + 1 - 2 * core
    long = is_long(me)
    barrier = pltpu.get_barrier_semaphore()
    load = pltpu.make_async_copy(amp_hbm, amp, a_sem)
    load.start()
    small = [
        pltpu.make_async_copy(blocks_hbm, blocks_ref, b_sem),
        pltpu.make_async_copy(counts_hbm, counts_ref, c_sem),
        pltpu.make_async_copy(fock_hbm, fock_ref, f_sem),
    ]
    for copy in small:
        copy.start()
    for d in range(1, NR):
        pl.semaphore_signal(barrier, inc=1, device_id={"row": (me + d) % NR}, device_id_type=MESH)
    pl.semaphore_signal(barrier, inc=1, device_id={"col": partner}, device_id_type=MESH)
    with jax.named_scope("load"):
        load.wait()

    with jax.named_scope("pack1"):
        for m in range(NR):
            for j, (x, y, h) in enumerate(pieces[m]):
                send1[pl.ds(m * S1 + j * SLOTS, SLOTS), :] = amp[x, y, :, pl.ds(h * LANES, LANES)]

    for copy in small:
        copy.wait()
    ftiles[0] = fock_ref[:8, :LANES]
    ftiles[1, :2] = fock_ref[8:, :LANES]
    ftiles[1, 2:8, :32] = fock_ref[:6, LANES:]
    ftiles[1, 2:6, 32:64] = fock_ref[6:, LANES:]

    with jax.named_scope("barrier"):
        pl.semaphore_wait(barrier, NR)

    def early1(to):
        return remote(
            send1.at[pl.ds(to * S1, ROWS1)], first1.at[pl.ds(me * R1 + FRONT, ROWS1)],
            s1_sem, r1_sem.at[0], {"row": to})

    def late1(to, rows):
        return remote(
            send1.at[pl.ds(to * S1 + ROWS1, rows)], second1.at[pl.ds(me * R1 + FRONT, rows)],
            s1_sem, r1_sem.at[1], {"row": to})

    def early2(to):
        return remote(
            send2.at[pl.ds(to * P2, ROWS2)], recv2.at[pl.ds(me * P2, ROWS2)],
            s2_sem, r2_sem.at[0], {"row": to})

    def late2(to, rows):
        return remote(
            send2.at[pl.ds(to * P2 + LATE, rows)], recv2.at[pl.ds(me * P2 + LATE, rows)],
            s2_sem, r2_sem.at[1], {"row": to})

    def fock_copy(to):
        return remote(ftiles.at[core], fgather.at[core, me], fs_sem, fr_sem, {"row": to})

    exchange = remote(fgather.at[core], fgather.at[core], ds_sem, dr_sem, {"col": partner})

    def both(flag, action):
        for value in (True, False):
            @pl.when(flag == value)
            def _():
                action(value)

    with jax.named_scope("start1"):
        @pl.loop(1, NR)
        def _(d):
            early1((me + d) % NR).start()

        @pl.loop(1, NR)
        def _(d):
            to = (me + d) % NR
            both(is_long(to), lambda value: late1(to, late_rows1(value)).start())

        @pl.loop(1, NR)
        def _(d):
            fock_copy((me + d) % NR).start()

    with jax.named_scope("tables"):
        first1[pl.ds(me * R1 + FRONT, ROWS1), :] = send1[pl.ds(me * S1, ROWS1), :]
        second1[pl.ds(me * R1 + FRONT, S1 - ROWS1), :] = send1[pl.ds(me * S1 + ROWS1, S1 - ROWS1), :]
        fgather[core, me] = ftiles[core]
        row = lax.broadcasted_iota(jnp.int32, (16, LANES), 0)
        is_pair = (row < 10) | ((row < 12) & (long | (me == 1) | (me == 14)))
        one = jnp.ones((16, LANES), jnp.float32)
        coef_a[0] = one
        coef_b[0] = jnp.zeros((16, LANES), jnp.float32)
        coef_a[1] = jnp.where(is_pair, 0.0, -one)
        coef_b[1] = jnp.where(is_pair, -one, 0.0)
        up_mask = (row % 2 == 0) & (row < 12)

        sub = lax.broadcasted_iota(jnp.int32, (8, LANES), 0)
        lane = lax.broadcasted_iota(jnp.int32, (8, LANES), 1)
        mine = ((sub % 2) * 8 + lane // NT - phase_ref[0] + NR) % NR
        other = (mine + lane) % NT
        low = jnp.minimum(mine, other)
        high = jnp.maximum(mine, other)
        ident = low * NT - (low * (low - 1)) // 2 + (high - low)

        def look(d, at):
            for slot in range(SLOTS):
                block = jnp.where(slot < counts_ref[d], blocks_ref[d, slot], -1)
                at = jnp.where(ident == block, d * R1 + (FRONT + slot), at)
            return at

        at = lax.fori_loop(0, NR, look, jnp.full((8, LANES), FRONT, jnp.int32))
        vtable[...] = jnp.where(sub < 2, at, jnp.where(other > mine, 1, 0))
        to_smem = pltpu.make_async_copy(vtable, table, t_sem)
        to_smem.start()
        to_smem.wait()

    def pack2(k, to, dst, slot):
        first = SPLIT * k
        n = SPLIT if k == 0 else 5
        base = slot * P2 + LATE * k
        recv1 = (first1, second1)[k]
        for c in range(NT):
            at = table[to // 8, (to % 8) * NT + c]
            if c == 0:
                dst[pl.ds(base, HEAD[k]), :] = recv1[pl.ds(at, HEAD[k], stride=2 * SLOTS), :]
                continue
            kind = table[2 + to // 8, (to % 8) * NT + c]
            v = recv1[pl.ds(at, n, stride=SLOTS), :]
            up = recv1[pl.ds(at + SLOTS, n, stride=SLOTS), :]
            down = recv1[pl.ds(at - SLOTS, n, stride=SLOTS), :]
            swapped = jnp.where(up_mask[first:first + n], up, down)
            dst[pl.ds(base + HEAD[k] + c - 1, n, stride=OTHERS), :] = (
                coef_a[kind, first:first + n] * v + coef_b[kind, first:first + n] * swapped)

    with jax.named_scope("wait1_0"):
        wait_rows(first1, OTHERS * ROWS1, r1_sem.at[0])

    with jax.named_scope("pack2_0"):
        @pl.loop(1, NR)
        def _(d):
            to = (me + d) % NR
            pack2(0, to, send2, to)
            early2(to).start()

        pack2(0, me, recv2, me)

    with jax.named_scope("wait1_1"):
        both(long, lambda value: wait_rows(second1, OTHERS * late_rows1(value), r1_sem.at[1]))

    with jax.named_scope("pack2_1"):
        @pl.loop(1, NR)
        def _(d):
            to = (me + d) % NR
            pack2(1, to, send2, to)
            both(long, lambda value: late2(to, late_rows2(value)).start())

        pack2(1, me, recv2, me)

    with jax.named_scope("waitf"):
        wait_rows(send1, OTHERS * 8, fr_sem)
        exchange.start()
        both(long, lambda value: wait_rows(
            send1, OTHERS * ROWS1 + (8 - value) * late_rows1(True) + (7 + value) * late_rows1(False), s1_sem))

    def assemble(first, last):
        for m in range(NR):
            for j, (x, y, h) in enumerate(pieces[m]):
                if not first <= j < last:
                    continue
                k = int(j >= SPLIT)
                base = m * P2 + LATE * k
                rows = recv2[pl.ds(base + HEAD[k] + (j - SPLIT * k) * OTHERS, OTHERS), :]
                dense[h, y, pl.ds(x + BT, OTHERS, stride=BT), :] = rows
                if x < y:
                    head = recv2[pl.ds(base + (j - SPLIT * k) // 2, 1), :]
                    dense[h, y, pl.ds(x, 1), :] = head
                    dense[h, x, pl.ds(y, 1), :] = -head
                elif x == y:
                    dense[h, y, pl.ds(x, 1), :] = jnp.zeros((1, LANES), jnp.float32)

    with jax.named_scope("wait2_0"):
        wait_rows(recv2, OTHERS * ROWS2, r2_sem.at[0])

    with jax.named_scope("assemble_0"):
        assemble(0, SPLIT)

    with jax.named_scope("fock"):
        exchange.wait()
        wait_rows(send1, OTHERS * 8, fs_sem)
        for d in range(NR):
            at = d * BT
            ffull[pl.ds(at, 8), :LANES] = fgather[0, d]
            ffull[pl.ds(at + 8, 2), :LANES] = fgather[1, d, :2]
            ffull[pl.ds(at, 6), LANES:] = fgather[1, d, 2:8, :32]
            ffull[pl.ds(at + 6, 4), LANES:] = fgather[1, d, 2:6, 32:64]
        turn = (me - phase_ref[0] + NR) % NR * BT
        size = NT * BT
        shifted = lax.broadcasted_iota(jnp.int32, (size, size), 1) + turn
        shifted = jnp.where(shifted >= size, shifted - size, shifted)
        picks = (lax.broadcasted_iota(jnp.int32, (size, size), 0) == shifted).astype(jnp.float32).astype(jnp.bfloat16)
        f = ffull[...]
        f_high = f.astype(jnp.bfloat16)
        f_low = (f - f_high.astype(jnp.float32)).astype(jnp.bfloat16)
        turned_high[...] = jnp.dot(f_high, picks, preferred_element_type=jnp.float32).astype(jnp.bfloat16)
        turned_low[...] = jnp.dot(f_low, picks, preferred_element_type=jnp.float32).astype(jnp.bfloat16)

    with jax.named_scope("wait2_1"):
        both(long, lambda value: wait_rows(
            recv2, (8 - value) * late_rows2(True) + (7 + value) * late_rows2(False), r2_sem.at[1]))

    with jax.named_scope("assemble_1"):
        assemble(SPLIT, 13)

    with jax.named_scope("matmul"):
        f_high = turned_high[...]
        f_low = turned_low[...]
        for y in range(BT):
            column = jnp.concatenate([dense[0, y], dense[1, y]], axis=1)
            c_high = column.astype(jnp.bfloat16)
            c_low = (column - c_high.astype(jnp.float32)).astype(jnp.bfloat16)
            out_ref[0, y] = (
                jnp.dot(f_high, c_high, preferred_element_type=jnp.float32)
                + jnp.dot(f_high, c_low, preferred_element_type=jnp.float32)
                + jnp.dot(f_low, c_high, preferred_element_type=jnp.float32))

    with jax.named_scope("drain"):
        both(long, lambda value: wait_rows(send2, OTHERS * (ROWS2 + late_rows2(value)), s2_sem))


def body(amplitudes, old_blocks, old_counts, new_phase, fock):
    nocc = amplitudes.shape[3]
    turned = jnp.transpose(amplitudes, (1, 2, 0, 3))
    hbm = pl.BlockSpec(memory_space=pltpu.HBM)
    operands = [
        pltpu.with_memory_space_constraint(array, pltpu.HBM)
        for array in (old_blocks, old_counts, turned, fock)
    ]
    size = NT * BT
    return pl.pallas_call(
        kernel,
        name="fock_two_phase",
        out_shape=jax.ShapeDtypeStruct((1, BT, size, nocc), jnp.float32),
        in_specs=[pl.BlockSpec(memory_space=pltpu.SMEM)] + [hbm] * 4,
        out_specs=pl.BlockSpec(memory_space=pltpu.VMEM),
        scratch_shapes=[
            pltpu.SMEM(old_blocks.shape, jnp.int32),
            pltpu.SMEM(old_counts.shape, jnp.int32),
            pltpu.VMEM(fock.shape, jnp.float32),
            pltpu.VMEM(turned.shape, jnp.float32),
            pltpu.VMEM((NR * S1, LANES), jnp.float32),
            pltpu.VMEM((NR * R1, LANES), jnp.float32),
            pltpu.VMEM((NR * R1, LANES), jnp.float32),
            pltpu.VMEM((NR * P2, LANES), jnp.float32),
            pltpu.VMEM((NR * P2, LANES), jnp.float32),
            pltpu.VMEM((2, 16, LANES), jnp.float32),
            pltpu.VMEM((2, 16, LANES), jnp.float32),
            pltpu.VMEM((2, 8, LANES), jnp.float32),
            pltpu.VMEM((2, NR, 8, LANES), jnp.float32),
            pltpu.VMEM((size, size), jnp.float32),
            pltpu.VMEM((size, size), jnp.bfloat16),
            pltpu.VMEM((size, size), jnp.bfloat16),
            pltpu.VMEM((2, BT, size, LANES), jnp.float32),
            pltpu.VMEM((8, LANES), jnp.int32),
            pltpu.SMEM((8, LANES), jnp.int32),
        ] + [pltpu.SemaphoreType.DMA] * 6 + [
            pltpu.SemaphoreType.DMA((2,)),
            pltpu.SemaphoreType.DMA,
            pltpu.SemaphoreType.DMA((2,)),
        ] + [pltpu.SemaphoreType.DMA] * 4,
        compiler_params=pltpu.CompilerParams(
            collective_id=0, has_side_effects=True, vmem_limit_bytes=48 << 20),
    )(new_phase, *operands)


def solution(mesh):
    return jax.shard_map(
        body,
        mesh=mesh,
        in_specs=(P("row", None, None, "col"), P(), P(), P(), P("row", None)),
        out_specs=P("row", None, None, "col"),
        check_vma=False,
    )
```

```python
import jax
import jax.numpy as jnp
from jax import lax
from jax.experimental import pallas as pl
from jax.experimental.pallas import tpu as pltpu
from jax.sharding import PartitionSpec as P

NT = 16
BT = 10
NR = 16
SLOTS = 12
LANES = 128
SPLIT = 8
EARLY = 4
TWO_EARLY = (1, 4, 11, 14)
TWO_LATE = (3, 12)
MESH = pl.DeviceIdType.MESH
S1 = 160
R1 = 128
FRONT = 16
P2 = 208
LATE = 128
OTHERS = NT - 1
HEAD = (SPLIT // 2, 2)
ROWS1 = SPLIT * SLOTS
ROWS2 = SPLIT * OTHERS + HEAD[0]


def is_long(m):
    return (m // 4 + m) % 2 == 0


def late_rows1(long):
    return (5 if long else 4) * SLOTS


def late_rows2(long):
    return (5 if long else 4) * OTHERS + HEAD[1]


def piece_tables():
    halves = range(2)
    pairs = [[], []]
    diagonal = [[], []]
    for h in halves:
        for x in range(BT):
            diagonal[x >= EARLY].append((x, x, h))
            pairs[x >= EARLY] += [(x, y, h) for y in range(x + 1, BT)]
    pieces = []
    for m in range(NR):
        rows = []
        for k, count, size in ((0, 3 if m in TWO_EARLY else 4, SPLIT), (1, 1 if m in TWO_LATE else 2, 13 if is_long(m) else 12)):
            for _ in range(count):
                x, y, h = pairs[k].pop(0)
                rows += [(x, y, h), (y, x, h)]
            while len(rows) < size:
                rows.append(diagonal[k].pop(0))
        pieces.append(rows)
    assert not any(pairs) and not any(diagonal)
    return pieces


def remote(src, dst, send, recv, to):
    return pltpu.make_async_remote_copy(
        src_ref=src, dst_ref=dst, send_sem=send, recv_sem=recv, device_id=to, device_id_type=MESH)


def wait_rows(ref, rows, sem):
    part = ref.at[pl.ds(0, rows)]
    pltpu.make_async_copy(part, part, sem).wait()


def contract(high_ref, low_ref, dense, columns, out):
    f_high = high_ref[...]
    f_low = low_ref[...]
    for y in columns:
        column = jnp.concatenate([dense[0, y], dense[1, y]], axis=1)
        c_high = column.astype(jnp.bfloat16)
        c_low = (column - c_high.astype(jnp.float32)).astype(jnp.bfloat16)
        out[y] = (
            jnp.dot(f_high, c_high, preferred_element_type=jnp.float32)
            + jnp.dot(f_high, c_low, preferred_element_type=jnp.float32)
            + jnp.dot(f_low, c_high, preferred_element_type=jnp.float32))


def kernel(
    phase_ref, blocks_hbm, counts_hbm, amp_hbm, fock_hbm, head_ref, dense, high_ref, low_ref,
    blocks_ref, counts_ref, fock_ref, amp, send1, first1, second1, send2, recv2, coef_a, coef_b,
    ftiles, fgather, ffull, early, vtable, table,
    a_sem, b_sem, c_sem, f_sem, t_sem, s1_sem, r1_sem, s2_sem, r2_sem, fs_sem, fr_sem, ds_sem, dr_sem,
):
    pieces = piece_tables()
    me = lax.axis_index("row")
    col = lax.axis_index("col")
    core = col % 2
    partner = col + 1 - 2 * core
    long = is_long(me)
    barrier = pltpu.get_barrier_semaphore()
    load = pltpu.make_async_copy(amp_hbm, amp, a_sem)
    load.start()
    small = [
        pltpu.make_async_copy(blocks_hbm, blocks_ref, b_sem),
        pltpu.make_async_copy(counts_hbm, counts_ref, c_sem),
        pltpu.make_async_copy(fock_hbm, fock_ref, f_sem),
    ]
    for copy in small:
        copy.start()
    for d in range(1, NR):
        pl.semaphore_signal(barrier, inc=1, device_id={"row": (me + d) % NR}, device_id_type=MESH)
    pl.semaphore_signal(barrier, inc=1, device_id={"col": partner}, device_id_type=MESH)
    with jax.named_scope("load"):
        load.wait()

    with jax.named_scope("pack1"):
        for m in range(NR):
            for j, (x, y, h) in enumerate(pieces[m]):
                send1[pl.ds(m * S1 + j * SLOTS, SLOTS), :] = amp[x, y, :, pl.ds(h * LANES, LANES)]

    for copy in small:
        copy.wait()
    ftiles[0] = fock_ref[:8, :LANES]
    ftiles[1, :2] = fock_ref[8:, :LANES]
    ftiles[1, 2:8, :32] = fock_ref[:6, LANES:]
    ftiles[1, 2:6, 32:64] = fock_ref[6:, LANES:]

    with jax.named_scope("barrier"):
        pl.semaphore_wait(barrier, NR)

    def early1(to):
        return remote(
            send1.at[pl.ds(to * S1, ROWS1)], first1.at[pl.ds(me * R1 + FRONT, ROWS1)],
            s1_sem, r1_sem.at[0], {"row": to})

    def late1(to, rows):
        return remote(
            send1.at[pl.ds(to * S1 + ROWS1, rows)], second1.at[pl.ds(me * R1 + FRONT, rows)],
            s1_sem, r1_sem.at[1], {"row": to})

    def early2(to):
        return remote(
            send2.at[pl.ds(to * P2, ROWS2)], recv2.at[pl.ds(me * P2, ROWS2)],
            s2_sem, r2_sem.at[0], {"row": to})

    def late2(to, rows):
        return remote(
            send2.at[pl.ds(to * P2 + LATE, rows)], recv2.at[pl.ds(me * P2 + LATE, rows)],
            s2_sem, r2_sem.at[1], {"row": to})

    def fock_copy(to):
        return remote(ftiles.at[core], fgather.at[core, me], fs_sem, fr_sem, {"row": to})

    exchange = remote(fgather.at[core], fgather.at[core], ds_sem, dr_sem, {"col": partner})

    def both(flag, action):
        for value in (True, False):
            @pl.when(flag == value)
            def _():
                action(value)

    with jax.named_scope("start1"):
        @pl.loop(1, NR)
        def _(d):
            early1((me + d) % NR).start()

        @pl.loop(1, NR)
        def _(d):
            to = (me + d) % NR
            both(is_long(to), lambda value: late1(to, late_rows1(value)).start())

        @pl.loop(1, NR)
        def _(d):
            fock_copy((me + d) % NR).start()

    with jax.named_scope("tables"):
        first1[pl.ds(me * R1 + FRONT, ROWS1), :] = send1[pl.ds(me * S1, ROWS1), :]
        second1[pl.ds(me * R1 + FRONT, S1 - ROWS1), :] = send1[pl.ds(me * S1 + ROWS1, S1 - ROWS1), :]
        fgather[core, me] = ftiles[core]
        row = lax.broadcasted_iota(jnp.int32, (16, LANES), 0)
        two_early = (me == 1) | (me == 4) | (me == 11) | (me == 14)
        two_late = (me == 3) | (me == 12)
        is_pair = (row < 12) & ~((row // 2 == 3) & two_early) & ~((row // 2 == 5) & two_late)
        one = jnp.ones((16, LANES), jnp.float32)
        coef_a[0] = one
        coef_b[0] = jnp.zeros((16, LANES), jnp.float32)
        coef_a[1] = jnp.where(is_pair, 0.0, -one)
        coef_b[1] = jnp.where(is_pair, -one, 0.0)
        up_mask = (row % 2 == 0) & (row < 12)

        sub = lax.broadcasted_iota(jnp.int32, (8, LANES), 0)
        lane = lax.broadcasted_iota(jnp.int32, (8, LANES), 1)
        mine = ((sub % 2) * 8 + lane // NT - phase_ref[0] + NR) % NR
        other = (mine + lane) % NT
        low = jnp.minimum(mine, other)
        high = jnp.maximum(mine, other)
        ident = low * NT - (low * (low - 1)) // 2 + (high - low)

        def look(d, at):
            for slot in range(SLOTS):
                block = jnp.where(slot < counts_ref[d], blocks_ref[d, slot], -1)
                at = jnp.where(ident == block, d * R1 + (FRONT + slot), at)
            return at

        at = lax.fori_loop(0, NR, look, jnp.full((8, LANES), FRONT, jnp.int32))
        vtable[...] = jnp.where(sub < 2, at, jnp.where(other > mine, 1, 0))
        to_smem = pltpu.make_async_copy(vtable, table, t_sem)
        to_smem.start()
        to_smem.wait()

    def pack2(k, to, dst, slot):
        first = SPLIT * k
        n = SPLIT if k == 0 else 5
        base = slot * P2 + LATE * k
        recv1 = (first1, second1)[k]
        for c in range(NT):
            at = table[to // 8, (to % 8) * NT + c]
            if c == 0:
                dst[pl.ds(base, HEAD[k]), :] = recv1[pl.ds(at, HEAD[k], stride=2 * SLOTS), :]
                continue
            kind = table[2 + to // 8, (to % 8) * NT + c]
            v = recv1[pl.ds(at, n, stride=SLOTS), :]
            up = recv1[pl.ds(at + SLOTS, n, stride=SLOTS), :]
            down = recv1[pl.ds(at - SLOTS, n, stride=SLOTS), :]
            swapped = jnp.where(up_mask[first:first + n], up, down)
            dst[pl.ds(base + HEAD[k] + c - 1, n, stride=OTHERS), :] = (
                coef_a[kind, first:first + n] * v + coef_b[kind, first:first + n] * swapped)

    with jax.named_scope("wait1_0"):
        wait_rows(first1, OTHERS * ROWS1, r1_sem.at[0])

    with jax.named_scope("pack2_0"):
        @pl.loop(1, NR)
        def _(d):
            to = (me + d) % NR
            pack2(0, to, send2, to)
            early2(to).start()

        pack2(0, me, recv2, me)

    with jax.named_scope("wait1_1"):
        both(long, lambda value: wait_rows(second1, OTHERS * late_rows1(value), r1_sem.at[1]))

    with jax.named_scope("pack2_1"):
        @pl.loop(1, NR)
        def _(d):
            to = (me + d) % NR
            pack2(1, to, send2, to)
            both(long, lambda value: late2(to, late_rows2(value)).start())

        pack2(1, me, recv2, me)

    with jax.named_scope("waitf"):
        wait_rows(send1, OTHERS * 8, fr_sem)
        exchange.start()
        both(long, lambda value: wait_rows(
            send1, OTHERS * ROWS1 + (8 - value) * late_rows1(True) + (7 + value) * late_rows1(False), s1_sem))

    def put(h, y, at, rows):
        target, column = (early, y) if y < EARLY else (dense, y - EARLY)
        target[h, column, at, :] = rows

    def assemble(first, last):
        for m in range(NR):
            for j, (x, y, h) in enumerate(pieces[m]):
                if not first <= j < last:
                    continue
                k = int(j >= SPLIT)
                base = m * P2 + LATE * k
                rows = recv2[pl.ds(base + HEAD[k] + (j - SPLIT * k) * OTHERS, OTHERS), :]
                put(h, y, pl.ds(x + BT, OTHERS, stride=BT), rows)
                if x < y:
                    head = recv2[pl.ds(base + (j - SPLIT * k) // 2, 1), :]
                    put(h, y, pl.ds(x, 1), head)
                    put(h, x, pl.ds(y, 1), -head)
                elif x == y:
                    put(h, y, pl.ds(x, 1), jnp.zeros((1, LANES), jnp.float32))

    with jax.named_scope("wait2_0"):
        wait_rows(recv2, OTHERS * ROWS2, r2_sem.at[0])

    with jax.named_scope("assemble_0"):
        assemble(0, SPLIT)

    with jax.named_scope("fock"):
        exchange.wait()
        wait_rows(send1, OTHERS * 8, fs_sem)
        for d in range(NR):
            at = d * BT
            ffull[pl.ds(at, 8), :LANES] = fgather[0, d]
            ffull[pl.ds(at + 8, 2), :LANES] = fgather[1, d, :2]
            ffull[pl.ds(at, 6), LANES:] = fgather[1, d, 2:8, :32]
            ffull[pl.ds(at + 6, 4), LANES:] = fgather[1, d, 2:6, 32:64]
        turn = (me - phase_ref[0] + NR) % NR * BT
        size = NT * BT
        shifted = lax.broadcasted_iota(jnp.int32, (size, size), 1) + turn
        shifted = jnp.where(shifted >= size, shifted - size, shifted)
        picks = (lax.broadcasted_iota(jnp.int32, (size, size), 0) == shifted).astype(jnp.float32).astype(jnp.bfloat16)
        f = ffull[...]
        f_high = f.astype(jnp.bfloat16)
        f_low = (f - f_high.astype(jnp.float32)).astype(jnp.bfloat16)
        high_ref[...] = jnp.dot(f_high, picks, preferred_element_type=jnp.float32).astype(jnp.bfloat16)
        low_ref[...] = jnp.dot(f_low, picks, preferred_element_type=jnp.float32).astype(jnp.bfloat16)

    with jax.named_scope("matmul_0"):
        contract(high_ref, low_ref, early, range(EARLY), head_ref)

    with jax.named_scope("wait2_1"):
        both(long, lambda value: wait_rows(
            recv2, (8 - value) * late_rows2(True) + (7 + value) * late_rows2(False), r2_sem.at[1]))

    with jax.named_scope("assemble_1"):
        assemble(SPLIT, 13)

    with jax.named_scope("drain"):
        both(long, lambda value: wait_rows(send2, OTHERS * (ROWS2 + late_rows2(value)), s2_sem))


def finish(head_ref, dense, high_ref, low_ref, out_hbm, late, h_sem, o_sem):
    copies = [pltpu.make_async_copy(head_ref, out_hbm.at[0, pl.ds(0, EARLY)], h_sem)]
    copies[0].start()
    for y in range(BT - EARLY):
        contract(high_ref, low_ref, dense, (y,), late)
        copies.append(pltpu.make_async_copy(late.at[y], out_hbm.at[0, EARLY + y], o_sem.at[y]))
        copies[-1].start()
    for copy in copies:
        copy.wait()


def body(amplitudes, old_blocks, old_counts, new_phase, fock):
    nocc = amplitudes.shape[3]
    turned = jnp.transpose(amplitudes, (1, 2, 0, 3))
    hbm = pl.BlockSpec(memory_space=pltpu.HBM)
    operands = [
        pltpu.with_memory_space_constraint(array, pltpu.HBM)
        for array in (old_blocks, old_counts, turned, fock)
    ]
    size = NT * BT
    vmem = pl.BlockSpec(memory_space=pltpu.VMEM)
    parts = pl.pallas_call(
        kernel,
        name="fock_two_phase",
        out_shape=(
            jax.ShapeDtypeStruct((EARLY, size, nocc), jnp.float32),
            jax.ShapeDtypeStruct((2, BT - EARLY, size, LANES), jnp.float32),
            jax.ShapeDtypeStruct((size, size), jnp.bfloat16),
            jax.ShapeDtypeStruct((size, size), jnp.bfloat16),
        ),
        in_specs=[pl.BlockSpec(memory_space=pltpu.SMEM)] + [hbm] * 4,
        out_specs=(vmem,) * 4,
        scratch_shapes=[
            pltpu.SMEM(old_blocks.shape, jnp.int32),
            pltpu.SMEM(old_counts.shape, jnp.int32),
            pltpu.VMEM(fock.shape, jnp.float32),
            pltpu.VMEM(turned.shape, jnp.float32),
            pltpu.VMEM((NR * S1, LANES), jnp.float32),
            pltpu.VMEM((NR * R1, LANES), jnp.float32),
            pltpu.VMEM((NR * R1, LANES), jnp.float32),
            pltpu.VMEM((NR * P2, LANES), jnp.float32),
            pltpu.VMEM((NR * P2, LANES), jnp.float32),
            pltpu.VMEM((2, 16, LANES), jnp.float32),
            pltpu.VMEM((2, 16, LANES), jnp.float32),
            pltpu.VMEM((2, 8, LANES), jnp.float32),
            pltpu.VMEM((2, NR, 8, LANES), jnp.float32),
            pltpu.VMEM((size, size), jnp.float32),
            pltpu.VMEM((2, EARLY, size, LANES), jnp.float32),
            pltpu.VMEM((8, LANES), jnp.int32),
            pltpu.SMEM((8, LANES), jnp.int32),
        ] + [pltpu.SemaphoreType.DMA] * 6 + [
            pltpu.SemaphoreType.DMA((2,)),
            pltpu.SemaphoreType.DMA,
            pltpu.SemaphoreType.DMA((2,)),
        ] + [pltpu.SemaphoreType.DMA] * 4,
        compiler_params=pltpu.CompilerParams(
            collective_id=0, has_side_effects=True, vmem_limit_bytes=48 << 20),
    )(new_phase, *operands)
    return pl.pallas_call(
        finish,
        name="fock_finish",
        out_shape=jax.ShapeDtypeStruct((1, BT, size, nocc), jnp.float32),
        in_specs=[vmem] * 4,
        out_specs=hbm,
        scratch_shapes=[
            pltpu.VMEM((BT - EARLY, size, nocc), jnp.float32),
            pltpu.SemaphoreType.DMA,
            pltpu.SemaphoreType.DMA((BT - EARLY,)),
        ],
        compiler_params=pltpu.CompilerParams(vmem_limit_bytes=16 << 20),
    )(*parts)


def solution(mesh):
    return jax.shard_map(
        body,
        mesh=mesh,
        in_specs=(P("row", None, None, "col"), P(), P(), P(), P("row", None)),
        out_specs=P("row", None, None, "col"),
        check_vma=False,
    )
```

```python
import jax
import jax.numpy as jnp
from jax import lax
from jax.experimental import pallas as pl
from jax.experimental.pallas import tpu as pltpu
from jax.sharding import PartitionSpec as P

NT = 16
BT = 10
NR = 16
NC = 8
SLOTS = 12
LANES = 128
SPLIT = 8
EARLY = 4
TWO_EARLY = (1, 4, 11, 14)
TWO_LATE = (3, 12)
MESH = pl.DeviceIdType.MESH
S1 = 160
R1 = 96
FRONT = 16
OTHERS = NT - 1
CUTS = (0, 4, 8, 13)
LAST = len(CUTS) - 2
MESH = pl.DeviceIdType.MESH
S1 = 160
R1 = 96
FRONT = 16
LATE = 128
OTHERS = NT - 1
HEAD = (SPLIT // 2, 2)
ROWS1 = SPLIT * SLOTS
ROWS2 = SPLIT * OTHERS + HEAD[0]


def is_long(m):
    return (m // 4 + m) % 2 == 0


def rows_in(k, long):
    return CUTS[k + 1] - CUTS[k] - int(k == LAST and not long)


def heads_in(k):
    return (CUTS[k + 1] - CUTS[k]) // 2


def rows1(k, long):
    return rows_in(k, long) * SLOTS


def rows2(k, long):
    return rows_in(k, long) * OTHERS + heads_in(k)


def base2(k):
    return sum(-(-rows2(i, True) // 8) * 8 for i in range(k))


P2 = base2(LAST + 1)


def piece_tables():
    halves = range(2)
    pairs = [[], []]
    diagonal = [[], []]
    for h in halves:
        for x in range(BT):
            diagonal[x >= EARLY].append((x, x, h))
            pairs[x >= EARLY] += [(x, y, h) for y in range(x + 1, BT)]
    pieces = []
    for m in range(NR):
        rows = []
        for k, count, size in ((0, 3 if m in TWO_EARLY else 4, SPLIT), (1, 1 if m in TWO_LATE else 2, 13 if is_long(m) else 12)):
            for _ in range(count):
                x, y, h = pairs[k].pop(0)
                rows += [(x, y, h), (y, x, h)]
            while len(rows) < size:
                rows.append(diagonal[k].pop(0))
        pieces.append(rows)
    assert not any(pairs) and not any(diagonal)
    return pieces


def remote(src, dst, send, recv, to):
    return pltpu.make_async_remote_copy(
        src_ref=src, dst_ref=dst, send_sem=send, recv_sem=recv, device_id=to, device_id_type=MESH)


def wait_rows(ref, rows, sem):
    part = ref.at[pl.ds(0, rows)]
    pltpu.make_async_copy(part, part, sem).wait()


def contract(high_ref, low_ref, dense, columns, out):
    f_high = high_ref[...]
    f_low = low_ref[...]
    for y in columns:
        column = jnp.concatenate([dense[0, y], dense[1, y]], axis=1)
        c_high = column.astype(jnp.bfloat16)
        c_low = (column - c_high.astype(jnp.float32)).astype(jnp.bfloat16)
        out[y] = (
            jnp.dot(f_high, c_high, preferred_element_type=jnp.float32)
            + jnp.dot(f_high, c_low, preferred_element_type=jnp.float32)
            + jnp.dot(f_low, c_high, preferred_element_type=jnp.float32))


def kernel(
    phase_hbm, blocks_hbm, counts_hbm, amp_hbm, fock_hbm, head_ref, dense, high_ref, low_ref,
    phase_ref, blocks_ref, counts_ref, fock_ref, amp, send1, land0, land1, land2, send2, recv2, coef_a, coef_b,
    ftiles, fgather, ffull, early, vtable, table,
    a_sem, p_sem, b_sem, c_sem, f_sem, t_sem, s1_sem, r1_sem, s2_sem, r2_sem, fs_sem, fr_sem, ds_sem, dr_sem,
):
    pieces = piece_tables()
    me = lax.axis_index("row")
    col = lax.axis_index("col")
    long = is_long(me)
    barrier = pltpu.get_barrier_semaphore()
    loads = [
        pltpu.make_async_copy(amp_hbm.at[part], amp.at[part], a_sem.at[i])
        for i, part in enumerate((
            (pl.ds(0, EARLY),),
            (pl.ds(EARLY, BT - EARLY), pl.ds(0, EARLY)),
            (pl.ds(EARLY, BT - EARLY), pl.ds(EARLY, BT - EARLY))))
    ]
    for copy in loads:
        copy.start()
    small = [
        pltpu.make_async_copy(phase_hbm, phase_ref, p_sem),
        pltpu.make_async_copy(blocks_hbm, blocks_ref, b_sem),
        pltpu.make_async_copy(counts_hbm, counts_ref, c_sem),
        pltpu.make_async_copy(fock_hbm, fock_ref, f_sem),
    ]
    for copy in small:
        copy.start()
    for d in range(1, NR):
        pl.semaphore_signal(barrier, inc=1, device_id={"row": (me + d) % NR}, device_id_type=MESH)
    for d in range(1, NC):
        pl.semaphore_signal(barrier, inc=1, device_id={"col": (col + d) % NC}, device_id_type=MESH)
    def pack1(first, last):
        for m in range(NR):
            for j, (x, y, h) in enumerate(pieces[m]):
                if first <= j < last:
                    send1[pl.ds(m * S1 + j * SLOTS, SLOTS), :] = amp[x, y, :, pl.ds(h * LANES, LANES)]

    with jax.named_scope("load"):
        loads[0].wait()
        loads[1].wait()
    with jax.named_scope("pack1_0"):
        pack1(0, SPLIT)
    with jax.named_scope("barrier"):
        pl.semaphore_wait(barrier, NR + NC - 2)

    lands = (land0, land1, land2)

    def send_1(k, to, rows):
        return remote(
            send1.at[pl.ds(to * S1 + CUTS[k] * SLOTS, rows)], lands[k].at[pl.ds(me * R1 + FRONT, rows)],
            s1_sem, r1_sem.at[k], {"row": to})

    def send_2(k, to, rows):
        at = base2(k)
        return remote(
            send2.at[pl.ds(to * P2 + at, rows)], recv2.at[pl.ds(me * P2 + at, rows)],
            s2_sem, r2_sem.at[k], {"row": to})

    def at_size(k, flag, action):
        if k == LAST:
            both(flag, action)
        else:
            action(True)

    def fock_copy(to):
        return remote(ftiles.at[col], fgather.at[col, me], fs_sem, fr_sem, {"row": to})

    def exchange(d):
        return remote(fgather.at[col], fgather.at[col], ds_sem, dr_sem, {"col": (col + d) % NC})

    def both(flag, action):
        for value in (True, False):
            @pl.when(flag == value)
            def _():
                action(value)

    def start1(k):
        @pl.loop(1, NR)
        def _(d):
            to = (me + d) % NR
            at_size(k, is_long(to), lambda value: send_1(k, to, rows1(k, value)).start())

    with jax.named_scope("start1"):
        for k in range(LAST):
            start1(k)

    with jax.named_scope("pack1_1"):
        loads[2].wait()
        pack1(SPLIT, 13)

    with jax.named_scope("start1b"):
        start1(LAST)

    for copy in small:
        copy.wait()
    for q in range(5):
        ftiles[q] = fock_ref[2 * q:2 * q + 2, :LANES]
    for q in range(5):
        ftiles[5 + q % 3, :, pl.ds(q // 3 * 32, 32)] = fock_ref[2 * q:2 * q + 2, LANES:]

    @pl.loop(1, NR)
    def _(d):
        fock_copy((me + d) % NR).start()

    with jax.named_scope("tables"):
        for k in range(LAST + 1):
            rows = rows1(k, True)
            lands[k][pl.ds(me * R1 + FRONT, rows), :] = send1[pl.ds(me * S1 + CUTS[k] * SLOTS, rows), :]
        fgather[col, me] = ftiles[col]
        row = lax.broadcasted_iota(jnp.int32, (16, LANES), 0)
        two_early = (me == 1) | (me == 4) | (me == 11) | (me == 14)
        two_late = (me == 3) | (me == 12)
        is_pair = (row < 12) & ~((row // 2 == 3) & two_early) & ~((row // 2 == 5) & two_late)
        one = jnp.ones((16, LANES), jnp.float32)
        coef_a[0] = one
        coef_b[0] = jnp.zeros((16, LANES), jnp.float32)
        coef_a[1] = jnp.where(is_pair, 0.0, -one)
        coef_b[1] = jnp.where(is_pair, -one, 0.0)
        up_mask = (row % 2 == 0) & (row < 12)

        sub = lax.broadcasted_iota(jnp.int32, (8, LANES), 0)
        lane = lax.broadcasted_iota(jnp.int32, (8, LANES), 1)
        mine = ((sub % 2) * 8 + lane // NT - phase_ref[0, 0] + NR) % NR
        other = (mine + lane) % NT
        low = jnp.minimum(mine, other)
        high = jnp.maximum(mine, other)
        ident = low * NT - (low * (low - 1)) // 2 + (high - low)

        def look(d, at):
            for slot in range(SLOTS):
                block = jnp.where(slot < counts_ref[d], blocks_ref[d, slot], -1)
                at = jnp.where(ident == block, d * R1 + (FRONT + slot), at)
            return at

        at = lax.fori_loop(0, NR, look, jnp.full((8, LANES), FRONT, jnp.int32))
        vtable[...] = jnp.where(sub < 2, at, jnp.where(other > mine, 1, 0))
        to_smem = pltpu.make_async_copy(vtable, table, t_sem)
        to_smem.start()
        to_smem.wait()

    def pack2(k, to, dst, slot):
        first = CUTS[k]
        n = CUTS[k + 1] - first
        base = slot * P2 + base2(k)
        land = lands[k]
        for c in range(NT):
            at = table[to // 8, (to % 8) * NT + c]
            if c == 0:
                dst[pl.ds(base, heads_in(k)), :] = land[pl.ds(at, heads_in(k), stride=2 * SLOTS), :]
                continue
            kind = table[2 + to // 8, (to % 8) * NT + c]
            v = land[pl.ds(at, n, stride=SLOTS), :]
            up = land[pl.ds(at + SLOTS, n, stride=SLOTS), :]
            down = land[pl.ds(at - SLOTS, n, stride=SLOTS), :]
            swapped = jnp.where(up_mask[first:first + n], up, down)
            dst[pl.ds(base + heads_in(k) + c - 1, n, stride=OTHERS), :] = (
                coef_a[kind, first:first + n] * v + coef_b[kind, first:first + n] * swapped)

    for k in range(LAST + 1):
        with jax.named_scope(f"wait1_{k}"):
            at_size(k, long, lambda value: wait_rows(lands[k], OTHERS * rows1(k, value), r1_sem.at[k]))

        with jax.named_scope(f"pack2_{k}"):
            @pl.loop(1, NR)
            def _(d):
                to = (me + d) % NR
                pack2(k, to, send2, to)
                at_size(k, long, lambda value: send_2(k, to, rows2(k, value)).start())

            pack2(k, me, recv2, me)

    with jax.named_scope("waitf"):
        wait_rows(send1, OTHERS * 2, fr_sem)
        for d in range(1, NC):
            exchange(d).start()
        both(long, lambda value: wait_rows(
            send1,
            OTHERS * CUTS[LAST] * SLOTS + (8 - value) * rows1(LAST, True) + (7 + value) * rows1(LAST, False),
            s1_sem))

    def put(h, y, at, rows):
        target, column = (early, y) if y < EARLY else (dense, y - EARLY)
        target[h, column, at, :] = rows

    def assemble(k):
        for m in range(NR):
            for j, (x, y, h) in enumerate(pieces[m]):
                if not CUTS[k] <= j < CUTS[k + 1]:
                    continue
                i = j - CUTS[k]
                base = m * P2 + base2(k)
                rows = recv2[pl.ds(base + heads_in(k) + i * OTHERS, OTHERS), :]
                put(h, y, pl.ds(x + BT, OTHERS, stride=BT), rows)
                if x < y:
                    head = recv2[pl.ds(base + i // 2, 1), :]
                    put(h, y, pl.ds(x, 1), head)
                    put(h, x, pl.ds(y, 1), -head)
                elif x == y:
                    put(h, y, pl.ds(x, 1), jnp.zeros((1, LANES), jnp.float32))

    for k in range(LAST):
        with jax.named_scope(f"wait2_{k}"):
            wait_rows(recv2, OTHERS * rows2(k, True), r2_sem.at[k])

        with jax.named_scope(f"assemble_{k}"):
            assemble(k)

    with jax.named_scope("fock"):
        wait_rows(send1, (NC - 1) * 2 * NR, dr_sem)
        wait_rows(send1, (NC - 1) * 2 * NR, ds_sem)
        wait_rows(send1, OTHERS * 2, fs_sem)
        for d in range(NR):
            for q in range(5):
                at = pl.ds(d * BT + 2 * q, 2)
                ffull[at, :LANES] = fgather[q, d]
                ffull[at, LANES:] = fgather[5 + q % 3, d, :, pl.ds(q // 3 * 32, 32)]
        turn = (me - phase_ref[0, 0] + NR) % NR * BT
        size = NT * BT
        shifted = lax.broadcasted_iota(jnp.int32, (size, size), 1) + turn
        shifted = jnp.where(shifted >= size, shifted - size, shifted)
        picks = (lax.broadcasted_iota(jnp.int32, (size, size), 0) == shifted).astype(jnp.float32).astype(jnp.bfloat16)
        f = ffull[...]
        f_high = f.astype(jnp.bfloat16)
        f_low = (f - f_high.astype(jnp.float32)).astype(jnp.bfloat16)
        high_ref[...] = jnp.dot(f_high, picks, preferred_element_type=jnp.float32).astype(jnp.bfloat16)
        low_ref[...] = jnp.dot(f_low, picks, preferred_element_type=jnp.float32).astype(jnp.bfloat16)

    with jax.named_scope("matmul_0"):
        contract(high_ref, low_ref, early, range(EARLY), head_ref)

    with jax.named_scope(f"wait2_{LAST}"):
        both(long, lambda value: wait_rows(
            recv2, (8 - value) * rows2(LAST, True) + (7 + value) * rows2(LAST, False), r2_sem.at[LAST]))

    with jax.named_scope(f"assemble_{LAST}"):
        assemble(LAST)

    with jax.named_scope("drain"):
        both(long, lambda value: wait_rows(send2, OTHERS * sum(rows2(k, value) for k in range(LAST + 1)), s2_sem))


def finish(head_ref, dense, high_ref, low_ref, out_hbm, late, h_sem, o_sem):
    copies = [pltpu.make_async_copy(head_ref, out_hbm.at[0, pl.ds(0, EARLY)], h_sem)]
    copies[0].start()
    for y in range(BT - EARLY):
        contract(high_ref, low_ref, dense, (y,), late)
        copies.append(pltpu.make_async_copy(late.at[y], out_hbm.at[0, EARLY + y], o_sem.at[y]))
        copies[-1].start()
    for copy in copies:
        copy.wait()


def body(amplitudes, old_blocks, old_counts, new_phase, fock):
    nocc = amplitudes.shape[3]
    turned = jnp.transpose(amplitudes, (1, 2, 0, 3))
    phase = new_phase.reshape(1, 1)
    hbm = pl.BlockSpec(memory_space=pltpu.HBM)
    operands = [
        pltpu.with_memory_space_constraint(array, pltpu.HBM)
        for array in (old_blocks, old_counts, turned, fock)
    ]
    size = NT * BT
    vmem = pl.BlockSpec(memory_space=pltpu.VMEM)
    parts = pl.pallas_call(
        kernel,
        name="fock_two_phase",
        out_shape=(
            jax.ShapeDtypeStruct((EARLY, size, nocc), jnp.float32),
            jax.ShapeDtypeStruct((2, BT - EARLY, size, LANES), jnp.float32),
            jax.ShapeDtypeStruct((size, size), jnp.bfloat16),
            jax.ShapeDtypeStruct((size, size), jnp.bfloat16),
        ),
        in_specs=[pl.BlockSpec(memory_space=pl.ANY)] + [hbm] * 4,
        out_specs=(vmem,) * 4,
        scratch_shapes=[
            pltpu.SMEM(phase.shape, jnp.int32),
            pltpu.SMEM(old_blocks.shape, jnp.int32),
            pltpu.SMEM(old_counts.shape, jnp.int32),
            pltpu.VMEM(fock.shape, jnp.float32),
            pltpu.VMEM(turned.shape, jnp.float32),
            pltpu.VMEM((NR * S1, LANES), jnp.float32),
            pltpu.VMEM((NR * R1, LANES), jnp.float32),
            pltpu.VMEM((NR * R1, LANES), jnp.float32),
            pltpu.VMEM((NR * R1, LANES), jnp.float32),
            pltpu.VMEM((NR * P2, LANES), jnp.float32),
            pltpu.VMEM((NR * P2, LANES), jnp.float32),
            pltpu.VMEM((2, 16, LANES), jnp.float32),
            pltpu.VMEM((2, 16, LANES), jnp.float32),
            pltpu.VMEM((NC, 2, LANES), jnp.float32),
            pltpu.VMEM((NC, NR, 2, LANES), jnp.float32),
            pltpu.VMEM((size, size), jnp.float32),
            pltpu.VMEM((2, EARLY, size, LANES), jnp.float32),
            pltpu.VMEM((8, LANES), jnp.int32),
            pltpu.SMEM((8, LANES), jnp.int32),
        ] + [pltpu.SemaphoreType.DMA((3,))] + [pltpu.SemaphoreType.DMA] * 6 + [
            pltpu.SemaphoreType.DMA((3,)),
            pltpu.SemaphoreType.DMA,
            pltpu.SemaphoreType.DMA((3,)),
        ] + [pltpu.SemaphoreType.DMA] * 4,
        compiler_params=pltpu.CompilerParams(
            collective_id=0, has_side_effects=True, vmem_limit_bytes=48 << 20),
    )(phase, *operands)
    return pl.pallas_call(
        finish,
        name="fock_finish",
        out_shape=jax.ShapeDtypeStruct((1, BT, size, nocc), jnp.float32),
        in_specs=[vmem] * 4,
        out_specs=hbm,
        scratch_shapes=[
            pltpu.VMEM((BT - EARLY, size, nocc), jnp.float32),
            pltpu.SemaphoreType.DMA,
            pltpu.SemaphoreType.DMA((BT - EARLY,)),
        ],
        compiler_params=pltpu.CompilerParams(vmem_limit_bytes=16 << 20),
    )(*parts)


def solution(mesh):
    return jax.shard_map(
        body,
        mesh=mesh,
        in_specs=(P("row", None, None, "col"), P(), P(), P(), P("row", None)),
        out_specs=P("row", None, None, "col"),
        check_vma=False,
    )
```

```python
import jax
import jax.numpy as jnp
from jax import lax
from jax.experimental import pallas as pl
from jax.experimental.pallas import tpu as pltpu
from jax.sharding import PartitionSpec as P

NT = 16
BT = 10
NR = 16
NC = 8
SLOTS = 12
LANES = 128
SPLIT = 8
EARLY = 4
TWO_EARLY = (1, 4, 11, 14)
TWO_LATE = (3, 12)
MESH = pl.DeviceIdType.MESH
S1 = 160
R1 = 96
FRONT = 16
OTHERS = NT - 1
CUTS = (0, 4, 8, 13)
LAST = len(CUTS) - 2


def is_long(m):
    return (m // 4 + m) % 2 == 0


def rows_in(k, long):
    return CUTS[k + 1] - CUTS[k] - int(k == LAST and not long)


def heads_in(k):
    return (CUTS[k + 1] - CUTS[k]) // 2


def rows1(k, long):
    return rows_in(k, long) * SLOTS


def rows2(k, long):
    return rows_in(k, long) * OTHERS + heads_in(k)


def base2(k):
    return sum(-(-rows2(i, True) // 8) * 8 for i in range(k))


P2 = base2(LAST + 1)


def piece_tables():
    halves = range(2)
    pairs = [[], []]
    diagonal = [[], []]
    for h in halves:
        for x in range(BT):
            diagonal[x >= EARLY].append((x, x, h))
            pairs[x >= EARLY] += [(x, y, h) for y in range(x + 1, BT)]
    pieces = []
    for m in range(NR):
        rows = []
        for k, count, size in ((0, 3 if m in TWO_EARLY else 4, SPLIT), (1, 1 if m in TWO_LATE else 2, 13 if is_long(m) else 12)):
            for _ in range(count):
                x, y, h = pairs[k].pop(0)
                rows += [(x, y, h), (y, x, h)]
            while len(rows) < size:
                rows.append(diagonal[k].pop(0))
        pieces.append(rows)
    assert not any(pairs) and not any(diagonal)
    return pieces


def remote(src, dst, send, recv, to):
    return pltpu.make_async_remote_copy(
        src_ref=src, dst_ref=dst, send_sem=send, recv_sem=recv, device_id=to, device_id_type=MESH)


def wait_rows(ref, rows, sem):
    part = ref.at[pl.ds(0, rows)]
    pltpu.make_async_copy(part, part, sem).wait()


def contract(f_ref, dense, columns, out):
    f = f_ref[...]
    for y in columns:
        column = jnp.concatenate([dense[0, y], dense[1, y]], axis=1)
        c_high = column.astype(jnp.bfloat16)
        c_low = (column - c_high.astype(jnp.float32)).astype(jnp.bfloat16)
        stack = jnp.concatenate([c_high, c_low, c_high], axis=0)
        out[y] = jnp.dot(f, stack, preferred_element_type=jnp.float32)


def kernel(
    phase_hbm, blocks_hbm, counts_hbm, amp_hbm, fock_hbm, head_ref, dense, f3_ref,
    phase_ref, blocks_ref, counts_ref, fock_ref, amp, send1, land0, land1, land2, send2, recv2, coef_a, coef_b,
    ftiles, fgather, ffull, early, vtable, table,
    a_sem, p_sem, b_sem, c_sem, f_sem, t_sem, s1_sem, r1_sem, s2_sem, r2_sem, fs_sem, fr_sem, ds_sem, dr_sem,
):
    pieces = piece_tables()
    me = lax.axis_index("row")
    col = lax.axis_index("col")
    long = is_long(me)
    barrier = pltpu.get_barrier_semaphore()
    loads = [
        pltpu.make_async_copy(amp_hbm.at[part], amp.at[part], a_sem.at[i])
        for i, part in enumerate((
            (pl.ds(0, EARLY),),
            (pl.ds(EARLY, BT - EARLY), pl.ds(0, EARLY)),
            (pl.ds(EARLY, BT - EARLY), pl.ds(EARLY, BT - EARLY))))
    ]
    for copy in loads:
        copy.start()
    small = [
        pltpu.make_async_copy(phase_hbm, phase_ref, p_sem),
        pltpu.make_async_copy(blocks_hbm, blocks_ref, b_sem),
        pltpu.make_async_copy(counts_hbm, counts_ref, c_sem),
        pltpu.make_async_copy(fock_hbm, fock_ref, f_sem),
    ]
    for copy in small:
        copy.start()
    for d in range(1, NR):
        pl.semaphore_signal(barrier, inc=1, device_id={"row": (me + d) % NR}, device_id_type=MESH)
    for d in range(1, NC):
        pl.semaphore_signal(barrier, inc=1, device_id={"col": (col + d) % NC}, device_id_type=MESH)
    def pack1(first, last):
        for m in range(NR):
            for j, (x, y, h) in enumerate(pieces[m]):
                if first <= j < last:
                    send1[pl.ds(m * S1 + j * SLOTS, SLOTS), :] = amp[x, y, :, pl.ds(h * LANES, LANES)]

    with jax.named_scope("load"):
        loads[0].wait()
        loads[1].wait()
    with jax.named_scope("pack1_0"):
        pack1(0, SPLIT)
    with jax.named_scope("barrier"):
        pl.semaphore_wait(barrier, NR + NC - 2)

    lands = (land0, land1, land2)

    def send_1(k, to, rows):
        return remote(
            send1.at[pl.ds(to * S1 + CUTS[k] * SLOTS, rows)], lands[k].at[pl.ds(me * R1 + FRONT, rows)],
            s1_sem, r1_sem.at[k], {"row": to})

    def send_2(k, to, rows):
        at = base2(k)
        return remote(
            send2.at[pl.ds(to * P2 + at, rows)], recv2.at[pl.ds(me * P2 + at, rows)],
            s2_sem, r2_sem.at[k], {"row": to})

    def at_size(k, flag, action):
        if k == LAST:
            both(flag, action)
        else:
            action(True)

    def fock_copy(to):
        return remote(ftiles.at[col], fgather.at[col, me], fs_sem, fr_sem, {"row": to})

    def exchange(d):
        return remote(fgather.at[col], fgather.at[col], ds_sem, dr_sem, {"col": (col + d) % NC})

    def both(flag, action):
        for value in (True, False):
            @pl.when(flag == value)
            def _():
                action(value)

    def start1(k):
        @pl.loop(1, NR)
        def _(d):
            to = (me + d) % NR
            at_size(k, is_long(to), lambda value: send_1(k, to, rows1(k, value)).start())

    with jax.named_scope("start1"):
        for k in range(LAST):
            start1(k)

    with jax.named_scope("pack1_1"):
        loads[2].wait()
        pack1(SPLIT, 13)

    with jax.named_scope("start1b"):
        start1(LAST)

    for copy in small:
        copy.wait()
    for q in range(5):
        ftiles[q] = fock_ref[2 * q:2 * q + 2, :LANES]
    for q in range(5):
        ftiles[5 + q % 3, :, pl.ds(q // 3 * 32, 32)] = fock_ref[2 * q:2 * q + 2, LANES:]

    @pl.loop(1, NR)
    def _(d):
        fock_copy((me + d) % NR).start()

    with jax.named_scope("tables"):
        for k in range(LAST + 1):
            rows = rows1(k, True)
            lands[k][pl.ds(me * R1 + FRONT, rows), :] = send1[pl.ds(me * S1 + CUTS[k] * SLOTS, rows), :]
        fgather[col, me] = ftiles[col]
        row = lax.broadcasted_iota(jnp.int32, (16, LANES), 0)
        two_early = (me == 1) | (me == 4) | (me == 11) | (me == 14)
        two_late = (me == 3) | (me == 12)
        is_pair = (row < 12) & ~((row // 2 == 3) & two_early) & ~((row // 2 == 5) & two_late)
        one = jnp.ones((16, LANES), jnp.float32)
        coef_a[0] = one
        coef_b[0] = jnp.zeros((16, LANES), jnp.float32)
        coef_a[1] = jnp.where(is_pair, 0.0, -one)
        coef_b[1] = jnp.where(is_pair, -one, 0.0)
        up_mask = (row % 2 == 0) & (row < 12)

        sub = lax.broadcasted_iota(jnp.int32, (8, LANES), 0)
        lane = lax.broadcasted_iota(jnp.int32, (8, LANES), 1)
        mine = ((sub % 2) * 8 + lane // NT - phase_ref[0, 0] + NR) % NR
        other = (mine + lane) % NT
        low = jnp.minimum(mine, other)
        high = jnp.maximum(mine, other)
        ident = low * NT - (low * (low - 1)) // 2 + (high - low)

        def look(d, at):
            for slot in range(SLOTS):
                block = jnp.where(slot < counts_ref[d], blocks_ref[d, slot], -1)
                at = jnp.where(ident == block, d * R1 + (FRONT + slot), at)
            return at

        at = lax.fori_loop(0, NR, look, jnp.full((8, LANES), FRONT, jnp.int32))
        vtable[...] = jnp.where(sub < 2, at, jnp.where(other > mine, 1, 0))
        to_smem = pltpu.make_async_copy(vtable, table, t_sem)
        to_smem.start()
        to_smem.wait()

    def pack2(k, to, dst, slot):
        first = CUTS[k]
        n = CUTS[k + 1] - first
        base = slot * P2 + base2(k)
        land = lands[k]
        for c in range(NT):
            at = table[to // 8, (to % 8) * NT + c]
            if c == 0:
                dst[pl.ds(base, heads_in(k)), :] = land[pl.ds(at, heads_in(k), stride=2 * SLOTS), :]
                continue
            kind = table[2 + to // 8, (to % 8) * NT + c]
            v = land[pl.ds(at, n, stride=SLOTS), :]
            up = land[pl.ds(at + SLOTS, n, stride=SLOTS), :]
            down = land[pl.ds(at - SLOTS, n, stride=SLOTS), :]
            swapped = jnp.where(up_mask[first:first + n], up, down)
            dst[pl.ds(base + heads_in(k) + c - 1, n, stride=OTHERS), :] = (
                coef_a[kind, first:first + n] * v + coef_b[kind, first:first + n] * swapped)

    for k in range(LAST + 1):
        with jax.named_scope(f"wait1_{k}"):
            at_size(k, long, lambda value: wait_rows(lands[k], OTHERS * rows1(k, value), r1_sem.at[k]))

        with jax.named_scope(f"pack2_{k}"):
            @pl.loop(1, NR)
            def _(d):
                to = (me + d) % NR
                pack2(k, to, send2, to)
                at_size(k, long, lambda value: send_2(k, to, rows2(k, value)).start())

            pack2(k, me, recv2, me)

    with jax.named_scope("waitf"):
        wait_rows(send1, OTHERS * 2, fr_sem)
        for d in range(1, NC):
            exchange(d).start()
        both(long, lambda value: wait_rows(
            send1,
            OTHERS * CUTS[LAST] * SLOTS + (8 - value) * rows1(LAST, True) + (7 + value) * rows1(LAST, False),
            s1_sem))

    def put(h, y, at, rows):
        target, column = (early, y) if y < EARLY else (dense, y - EARLY)
        target[h, column, at, :] = rows

    def assemble(k):
        for m in range(NR):
            for j, (x, y, h) in enumerate(pieces[m]):
                if not CUTS[k] <= j < CUTS[k + 1]:
                    continue
                i = j - CUTS[k]
                base = m * P2 + base2(k)
                rows = recv2[pl.ds(base + heads_in(k) + i * OTHERS, OTHERS), :]
                put(h, y, pl.ds(x + BT, OTHERS, stride=BT), rows)
                if x < y:
                    head = recv2[pl.ds(base + i // 2, 1), :]
                    put(h, y, pl.ds(x, 1), head)
                    put(h, x, pl.ds(y, 1), -head)
                elif x == y:
                    put(h, y, pl.ds(x, 1), jnp.zeros((1, LANES), jnp.float32))

    for k in range(LAST):
        with jax.named_scope(f"wait2_{k}"):
            wait_rows(recv2, OTHERS * rows2(k, True), r2_sem.at[k])

        with jax.named_scope(f"assemble_{k}"):
            assemble(k)

    with jax.named_scope("fock"):
        wait_rows(send1, (NC - 1) * 2 * NR, dr_sem)
        wait_rows(send1, (NC - 1) * 2 * NR, ds_sem)
        wait_rows(send1, OTHERS * 2, fs_sem)
        for d in range(NR):
            for q in range(5):
                at = pl.ds(d * BT + 2 * q, 2)
                ffull[at, :LANES] = fgather[q, d]
                ffull[at, LANES:] = fgather[5 + q % 3, d, :, pl.ds(q // 3 * 32, 32)]
        turn = (me - phase_ref[0, 0] + NR) % NR * BT
        size = NT * BT
        wide = lax.broadcasted_iota(jnp.int32, (size, 3 * size), 1)
        part = (wide >= size).astype(jnp.int32) + (wide >= 2 * size).astype(jnp.int32)
        shifted = wide - part * size + turn
        shifted = jnp.where(shifted >= size, shifted - size, shifted)
        picks = (lax.broadcasted_iota(jnp.int32, (size, 3 * size), 0) == shifted).astype(jnp.float32)
        f = ffull[...]
        f_high = f.astype(jnp.bfloat16)
        f_low = (f - f_high.astype(jnp.float32)).astype(jnp.bfloat16)
        f3_ref[...] = (
            jnp.dot(f_high, jnp.where(part < 2, picks, 0.0).astype(jnp.bfloat16), preferred_element_type=jnp.float32)
            + jnp.dot(f_low, jnp.where(part == 2, picks, 0.0).astype(jnp.bfloat16), preferred_element_type=jnp.float32)
        ).astype(jnp.bfloat16)

    with jax.named_scope("matmul_0"):
        contract(f3_ref, early, range(EARLY), head_ref)

    with jax.named_scope(f"wait2_{LAST}"):
        both(long, lambda value: wait_rows(
            recv2, (8 - value) * rows2(LAST, True) + (7 + value) * rows2(LAST, False), r2_sem.at[LAST]))

    with jax.named_scope(f"assemble_{LAST}"):
        assemble(LAST)

    with jax.named_scope("drain"):
        both(long, lambda value: wait_rows(send2, OTHERS * sum(rows2(k, value) for k in range(LAST + 1)), s2_sem))


def finish(head_ref, dense, f3_ref, out_hbm, late, h_sem, o_sem):
    copies = [pltpu.make_async_copy(head_ref, out_hbm.at[0, pl.ds(0, EARLY)], h_sem)]
    copies[0].start()
    for y in range(BT - EARLY):
        contract(f3_ref, dense, (y,), late)
        copies.append(pltpu.make_async_copy(late.at[y], out_hbm.at[0, EARLY + y], o_sem.at[y]))
        copies[-1].start()
    for copy in copies:
        copy.wait()


def body(amplitudes, old_blocks, old_counts, new_phase, fock):
    nocc = amplitudes.shape[3]
    turned = jnp.transpose(amplitudes, (1, 2, 0, 3))
    phase = new_phase.reshape(1, 1)
    hbm = pl.BlockSpec(memory_space=pltpu.HBM)
    operands = [
        pltpu.with_memory_space_constraint(array, pltpu.HBM)
        for array in (old_blocks, old_counts, turned, fock)
    ]
    size = NT * BT
    vmem = pl.BlockSpec(memory_space=pltpu.VMEM)
    parts = pl.pallas_call(
        kernel,
        name="fock_two_phase",
        out_shape=(
            jax.ShapeDtypeStruct((EARLY, size, nocc), jnp.float32),
            jax.ShapeDtypeStruct((2, BT - EARLY, size, LANES), jnp.float32),
            jax.ShapeDtypeStruct((size, 3 * size), jnp.bfloat16),
        ),
        in_specs=[pl.BlockSpec(memory_space=pl.ANY)] + [hbm] * 4,
        out_specs=(vmem,) * 3,
        scratch_shapes=[
            pltpu.SMEM(phase.shape, jnp.int32),
            pltpu.SMEM(old_blocks.shape, jnp.int32),
            pltpu.SMEM(old_counts.shape, jnp.int32),
            pltpu.VMEM(fock.shape, jnp.float32),
            pltpu.VMEM(turned.shape, jnp.float32),
            pltpu.VMEM((NR * S1, LANES), jnp.float32),
            pltpu.VMEM((NR * R1, LANES), jnp.float32),
            pltpu.VMEM((NR * R1, LANES), jnp.float32),
            pltpu.VMEM((NR * R1, LANES), jnp.float32),
            pltpu.VMEM((NR * P2, LANES), jnp.float32),
            pltpu.VMEM((NR * P2, LANES), jnp.float32),
            pltpu.VMEM((2, 16, LANES), jnp.float32),
            pltpu.VMEM((2, 16, LANES), jnp.float32),
            pltpu.VMEM((NC, 2, LANES), jnp.float32),
            pltpu.VMEM((NC, NR, 2, LANES), jnp.float32),
            pltpu.VMEM((size, size), jnp.float32),
            pltpu.VMEM((2, EARLY, size, LANES), jnp.float32),
            pltpu.VMEM((8, LANES), jnp.int32),
            pltpu.SMEM((8, LANES), jnp.int32),
        ] + [pltpu.SemaphoreType.DMA((3,))] + [pltpu.SemaphoreType.DMA] * 6 + [
            pltpu.SemaphoreType.DMA((3,)),
            pltpu.SemaphoreType.DMA,
            pltpu.SemaphoreType.DMA((3,)),
        ] + [pltpu.SemaphoreType.DMA] * 4,
        compiler_params=pltpu.CompilerParams(
            collective_id=0, has_side_effects=True, vmem_limit_bytes=48 << 20),
    )(phase, *operands)
    return pl.pallas_call(
        finish,
        name="fock_finish",
        out_shape=jax.ShapeDtypeStruct((1, BT, size, nocc), jnp.float32),
        in_specs=[vmem] * 3,
        out_specs=hbm,
        scratch_shapes=[
            pltpu.VMEM((BT - EARLY, size, nocc), jnp.float32),
            pltpu.SemaphoreType.DMA,
            pltpu.SemaphoreType.DMA((BT - EARLY,)),
        ],
        compiler_params=pltpu.CompilerParams(vmem_limit_bytes=16 << 20),
    )(*parts)


def solution(mesh):
    return jax.shard_map(
        body,
        mesh=mesh,
        in_specs=(P("row", None, None, "col"), P(), P(), P(), P("row", None)),
        out_specs=P("row", None, None, "col"),
        check_vma=False,
    )
```

```python
import jax
import jax.numpy as jnp
from jax import lax
from jax.experimental import pallas as pl
from jax.experimental.pallas import tpu as pltpu
from jax.sharding import PartitionSpec as P

NT = 16
BT = 10
NR = 16
NC = 8
SLOTS = 12
LANES = 128
SPLIT = 8
EARLY = 4
TWO_EARLY = (1, 4, 11, 14)
TWO_LATE = (3, 12)
MESH = pl.DeviceIdType.MESH
S1 = 160
R1 = 96
FRONT = 16
OTHERS = NT - 1
CUTS = (0, 4, 8, 13)
LAST = len(CUTS) - 2


def is_long(m):
    return (m // 4 + m) % 2 == 0


def rows_in(k, long):
    return CUTS[k + 1] - CUTS[k] - int(k == LAST and not long)


def heads_in(k):
    return (CUTS[k + 1] - CUTS[k]) // 2


def rows1(k, long):
    return rows_in(k, long) * SLOTS


def rows2(k, long):
    return rows_in(k, long) * OTHERS + heads_in(k)


def base2(k):
    return sum(-(-rows2(i, True) // 8) * 8 for i in range(k))


P2 = base2(LAST + 1)


def piece_tables():
    halves = range(2)
    pairs = [[], []]
    diagonal = [[], []]
    for h in halves:
        for x in range(BT):
            diagonal[x >= EARLY].append((x, x, h))
            pairs[x >= EARLY] += [(x, y, h) for y in range(x + 1, BT)]
    pieces = []
    for m in range(NR):
        rows = []
        for k, count, size in ((0, 3 if m in TWO_EARLY else 4, SPLIT), (1, 1 if m in TWO_LATE else 2, 13 if is_long(m) else 12)):
            for _ in range(count):
                x, y, h = pairs[k].pop(0)
                rows += [(x, y, h), (y, x, h)]
            while len(rows) < size:
                rows.append(diagonal[k].pop(0))
        pieces.append(rows)
    assert not any(pairs) and not any(diagonal)
    return pieces


def remote(src, dst, send, recv, to):
    return pltpu.make_async_remote_copy(
        src_ref=src, dst_ref=dst, send_sem=send, recv_sem=recv, device_id=to, device_id_type=MESH)


def wait_rows(ref, rows, sem):
    part = ref.at[pl.ds(0, rows)]
    pltpu.make_async_copy(part, part, sem).wait()


def contract(f_ref, dense, columns, out):
    f = f_ref[...]
    for y in columns:
        column = jnp.concatenate([dense[0, y], dense[1, y]], axis=1)
        c_high = column.astype(jnp.bfloat16)
        c_low = (column - c_high.astype(jnp.float32)).astype(jnp.bfloat16)
        stack = jnp.concatenate([c_high, c_low, c_high], axis=0)
        out[y] = jnp.dot(f, stack, preferred_element_type=jnp.float32)


def kernel(
    phase_hbm, blocks_hbm, counts_hbm, amp_hbm, fock_hbm, head_ref, dense, f3_ref,
    phase_ref, blocks_ref, counts_ref, fock_ref, amp, send1, land0, land1, land2, send2, recv2, coef_a, coef_b,
    ftiles, fgather, ffull, early, vtable, table,
    a_sem, p_sem, b_sem, c_sem, f_sem, t_sem, s1_sem, r1_sem, s2_sem, r2_sem, fs_sem, fr_sem, ds_sem, dr_sem,
):
    pieces = piece_tables()
    me = lax.axis_index("row")
    col = lax.axis_index("col")
    long = is_long(me)
    barrier = pltpu.get_barrier_semaphore()
    for d in (10, 9, 11, 6, 14, 7, 5, 13, 15, 8, 2, 3, 12, 4, 1):
        pl.semaphore_signal(barrier, inc=1, device_id={"row": (me + d) % NR}, device_id_type=MESH)
    for d in range(1, NC):
        pl.semaphore_signal(barrier, inc=1, device_id={"col": (col + d) % NC}, device_id_type=MESH)
    loads = [
        pltpu.make_async_copy(amp_hbm.at[part], amp.at[part], a_sem.at[i])
        for i, part in enumerate((
            (pl.ds(0, EARLY),),
            (pl.ds(EARLY, BT - EARLY), pl.ds(0, EARLY)),
            (pl.ds(EARLY, BT - EARLY), pl.ds(EARLY, BT - EARLY))))
    ]
    for copy in loads:
        copy.start()
    small = [
        pltpu.make_async_copy(phase_hbm, phase_ref, p_sem),
        pltpu.make_async_copy(blocks_hbm, blocks_ref, b_sem),
        pltpu.make_async_copy(counts_hbm, counts_ref, c_sem),
        pltpu.make_async_copy(fock_hbm, fock_ref, f_sem),
    ]
    for copy in small:
        copy.start()

    def pack1(first, last):
        for m in range(NR):
            for j, (x, y, h) in enumerate(pieces[m]):
                if first <= j < last:
                    send1[pl.ds(m * S1 + j * SLOTS, SLOTS), :] = amp[x, y, :, pl.ds(h * LANES, LANES)]

    with jax.named_scope("load"):
        loads[0].wait()
        loads[1].wait()
    with jax.named_scope("pack1_0"):
        pack1(0, SPLIT)
    with jax.named_scope("barrier"):
        pl.semaphore_wait(barrier, NR + NC - 2)

    lands = (land0, land1, land2)

    def send_1(k, to, rows):
        return remote(
            send1.at[pl.ds(to * S1 + CUTS[k] * SLOTS, rows)], lands[k].at[pl.ds(me * R1 + FRONT, rows)],
            s1_sem, r1_sem.at[k], {"row": to})

    def send_2(k, to, rows):
        at = base2(k)
        return remote(
            send2.at[pl.ds(to * P2 + at, rows)], recv2.at[pl.ds(me * P2 + at, rows)],
            s2_sem, r2_sem.at[k], {"row": to})

    def at_size(k, flag, action):
        if k == LAST:
            both(flag, action)
        else:
            action(True)

    def fock_copy(to):
        return remote(ftiles.at[col], fgather.at[col, me], fs_sem, fr_sem, {"row": to})

    def exchange(d):
        return remote(fgather.at[col], fgather.at[col], ds_sem, dr_sem, {"col": (col + d) % NC})

    def both(flag, action):
        for value in (True, False):
            @pl.when(flag == value)
            def _():
                action(value)

    def start1(k):
        @pl.loop(1, NR)
        def _(d):
            to = (me + d) % NR
            at_size(k, is_long(to), lambda value: send_1(k, to, rows1(k, value)).start())

    with jax.named_scope("start1"):
        for k in range(LAST):
            start1(k)

    with jax.named_scope("pack1_1"):
        loads[2].wait()
        pack1(SPLIT, 13)

    with jax.named_scope("start1b"):
        start1(LAST)

    for copy in small:
        copy.wait()
    for q in range(5):
        ftiles[q] = fock_ref[2 * q:2 * q + 2, :LANES]
    for q in range(5):
        ftiles[5 + q % 3, :, pl.ds(q // 3 * 32, 32)] = fock_ref[2 * q:2 * q + 2, LANES:]

    @pl.loop(1, NR)
    def _(d):
        fock_copy((me + d) % NR).start()

    with jax.named_scope("tables"):
        for k in range(LAST + 1):
            rows = rows1(k, True)
            lands[k][pl.ds(me * R1 + FRONT, rows), :] = send1[pl.ds(me * S1 + CUTS[k] * SLOTS, rows), :]
        fgather[col, me] = ftiles[col]
        row = lax.broadcasted_iota(jnp.int32, (16, LANES), 0)
        two_early = (me == 1) | (me == 4) | (me == 11) | (me == 14)
        two_late = (me == 3) | (me == 12)
        is_pair = (row < 12) & ~((row // 2 == 3) & two_early) & ~((row // 2 == 5) & two_late)
        one = jnp.ones((16, LANES), jnp.float32)
        coef_a[0] = one
        coef_b[0] = jnp.zeros((16, LANES), jnp.float32)
        coef_a[1] = jnp.where(is_pair, 0.0, -one)
        coef_b[1] = jnp.where(is_pair, -one, 0.0)
        up_mask = (row % 2 == 0) & (row < 12)

        sub = lax.broadcasted_iota(jnp.int32, (8, LANES), 0)
        lane = lax.broadcasted_iota(jnp.int32, (8, LANES), 1)
        mine = ((sub % 2) * 8 + lane // NT - phase_ref[0, 0] + NR) % NR
        other = (mine + lane) % NT
        low = jnp.minimum(mine, other)
        high = jnp.maximum(mine, other)
        ident = low * NT - (low * (low - 1)) // 2 + (high - low)

        def look(d, at):
            for slot in range(SLOTS):
                block = jnp.where(slot < counts_ref[d], blocks_ref[d, slot], -1)
                at = jnp.where(ident == block, d * R1 + (FRONT + slot), at)
            return at

        at = lax.fori_loop(0, NR, look, jnp.full((8, LANES), FRONT, jnp.int32))
        vtable[...] = jnp.where(sub < 2, at, jnp.where(other > mine, 1, 0))
        to_smem = pltpu.make_async_copy(vtable, table, t_sem)
        to_smem.start()
        to_smem.wait()

    def pack2(k, to, dst, slot):
        first = CUTS[k]
        n = CUTS[k + 1] - first
        base = slot * P2 + base2(k)
        land = lands[k]
        for c in range(NT):
            at = table[to // 8, (to % 8) * NT + c]
            if c == 0:
                dst[pl.ds(base, heads_in(k)), :] = land[pl.ds(at, heads_in(k), stride=2 * SLOTS), :]
                continue
            kind = table[2 + to // 8, (to % 8) * NT + c]
            v = land[pl.ds(at, n, stride=SLOTS), :]
            up = land[pl.ds(at + SLOTS, n, stride=SLOTS), :]
            down = land[pl.ds(at - SLOTS, n, stride=SLOTS), :]
            swapped = jnp.where(up_mask[first:first + n], up, down)
            dst[pl.ds(base + heads_in(k) + c - 1, n, stride=OTHERS), :] = (
                coef_a[kind, first:first + n] * v + coef_b[kind, first:first + n] * swapped)

    for k in range(LAST + 1):
        with jax.named_scope(f"wait1_{k}"):
            at_size(k, long, lambda value: wait_rows(lands[k], OTHERS * rows1(k, value), r1_sem.at[k]))

        with jax.named_scope(f"pack2_{k}"):
            @pl.loop(1, NR)
            def _(d):
                to = (me + d) % NR
                pack2(k, to, send2, to)
                at_size(k, long, lambda value: send_2(k, to, rows2(k, value)).start())

            pack2(k, me, recv2, me)

    with jax.named_scope("waitf"):
        wait_rows(send1, OTHERS * 2, fr_sem)
        for d in range(1, NC):
            exchange(d).start()
        both(long, lambda value: wait_rows(
            send1,
            OTHERS * CUTS[LAST] * SLOTS + (8 - value) * rows1(LAST, True) + (7 + value) * rows1(LAST, False),
            s1_sem))

    def put(h, y, at, rows):
        target, column = (early, y) if y < EARLY else (dense, y - EARLY)
        target[h, column, at, :] = rows

    def assemble(k):
        for m in range(NR):
            for j, (x, y, h) in enumerate(pieces[m]):
                if not CUTS[k] <= j < CUTS[k + 1]:
                    continue
                i = j - CUTS[k]
                base = m * P2 + base2(k)
                rows = recv2[pl.ds(base + heads_in(k) + i * OTHERS, OTHERS), :]
                put(h, y, pl.ds(x + BT, OTHERS, stride=BT), rows)
                if x < y:
                    head = recv2[pl.ds(base + i // 2, 1), :]
                    put(h, y, pl.ds(x, 1), head)
                    put(h, x, pl.ds(y, 1), -head)
                elif x == y:
                    put(h, y, pl.ds(x, 1), jnp.zeros((1, LANES), jnp.float32))

    for k in range(LAST):
        with jax.named_scope(f"wait2_{k}"):
            wait_rows(recv2, OTHERS * rows2(k, True), r2_sem.at[k])

        with jax.named_scope(f"assemble_{k}"):
            assemble(k)

    with jax.named_scope("fock"):
        wait_rows(send1, (NC - 1) * 2 * NR, dr_sem)
        wait_rows(send1, (NC - 1) * 2 * NR, ds_sem)
        wait_rows(send1, OTHERS * 2, fs_sem)
        for d in range(NR):
            for q in range(5):
                at = pl.ds(d * BT + 2 * q, 2)
                ffull[at, :LANES] = fgather[q, d]
                ffull[at, LANES:] = fgather[5 + q % 3, d, :, pl.ds(q // 3 * 32, 32)]
        turn = (me - phase_ref[0, 0] + NR) % NR * BT
        size = NT * BT
        wide = lax.broadcasted_iota(jnp.int32, (size, 3 * size), 1)
        part = (wide >= size).astype(jnp.int32) + (wide >= 2 * size).astype(jnp.int32)
        shifted = wide - part * size + turn
        shifted = jnp.where(shifted >= size, shifted - size, shifted)
        picks = (lax.broadcasted_iota(jnp.int32, (size, 3 * size), 0) == shifted).astype(jnp.float32)
        f = ffull[...]
        f_high = f.astype(jnp.bfloat16)
        f_low = (f - f_high.astype(jnp.float32)).astype(jnp.bfloat16)
        f3_ref[...] = (
            jnp.dot(f_high, jnp.where(part < 2, picks, 0.0).astype(jnp.bfloat16), preferred_element_type=jnp.float32)
            + jnp.dot(f_low, jnp.where(part == 2, picks, 0.0).astype(jnp.bfloat16), preferred_element_type=jnp.float32)
        ).astype(jnp.bfloat16)

    with jax.named_scope("matmul_0"):
        contract(f3_ref, early, range(EARLY), head_ref)

    with jax.named_scope(f"wait2_{LAST}"):
        both(long, lambda value: wait_rows(
            recv2, (8 - value) * rows2(LAST, True) + (7 + value) * rows2(LAST, False), r2_sem.at[LAST]))

    with jax.named_scope(f"assemble_{LAST}"):
        assemble(LAST)

    with jax.named_scope("drain"):
        both(long, lambda value: wait_rows(send2, OTHERS * sum(rows2(k, value) for k in range(LAST + 1)), s2_sem))


def finish(head_ref, dense, f3_ref, out_hbm, late, h_sem, o_sem):
    copies = [pltpu.make_async_copy(head_ref, out_hbm.at[0, pl.ds(0, EARLY)], h_sem)]
    copies[0].start()
    for y in range(BT - EARLY):
        contract(f3_ref, dense, (y,), late)
        copies.append(pltpu.make_async_copy(late.at[y], out_hbm.at[0, EARLY + y], o_sem.at[y]))
        copies[-1].start()
    for copy in copies:
        copy.wait()


def body(amplitudes, old_blocks, old_counts, new_phase, fock):
    nocc = amplitudes.shape[3]
    turned = jnp.transpose(amplitudes, (1, 2, 0, 3))
    phase = new_phase.reshape(1, 1)
    hbm = pl.BlockSpec(memory_space=pltpu.HBM)
    operands = [
        pltpu.with_memory_space_constraint(array, pltpu.HBM)
        for array in (old_blocks, old_counts, turned, fock)
    ]
    size = NT * BT
    vmem = pl.BlockSpec(memory_space=pltpu.VMEM)
    parts = pl.pallas_call(
        kernel,
        name="fock_two_phase",
        out_shape=(
            jax.ShapeDtypeStruct((EARLY, size, nocc), jnp.float32),
            jax.ShapeDtypeStruct((2, BT - EARLY, size, LANES), jnp.float32),
            jax.ShapeDtypeStruct((size, 3 * size), jnp.bfloat16),
        ),
        in_specs=[pl.BlockSpec(memory_space=pl.ANY)] + [hbm] * 4,
        out_specs=(vmem,) * 3,
        scratch_shapes=[
            pltpu.SMEM(phase.shape, jnp.int32),
            pltpu.SMEM(old_blocks.shape, jnp.int32),
            pltpu.SMEM(old_counts.shape, jnp.int32),
            pltpu.VMEM(fock.shape, jnp.float32),
            pltpu.VMEM(turned.shape, jnp.float32),
            pltpu.VMEM((NR * S1, LANES), jnp.float32),
            pltpu.VMEM((NR * R1, LANES), jnp.float32),
            pltpu.VMEM((NR * R1, LANES), jnp.float32),
            pltpu.VMEM((NR * R1, LANES), jnp.float32),
            pltpu.VMEM((NR * P2, LANES), jnp.float32),
            pltpu.VMEM((NR * P2, LANES), jnp.float32),
            pltpu.VMEM((2, 16, LANES), jnp.float32),
            pltpu.VMEM((2, 16, LANES), jnp.float32),
            pltpu.VMEM((NC, 2, LANES), jnp.float32),
            pltpu.VMEM((NC, NR, 2, LANES), jnp.float32),
            pltpu.VMEM((size, size), jnp.float32),
            pltpu.VMEM((2, EARLY, size, LANES), jnp.float32),
            pltpu.VMEM((8, LANES), jnp.int32),
            pltpu.SMEM((8, LANES), jnp.int32),
        ] + [pltpu.SemaphoreType.DMA((3,))] + [pltpu.SemaphoreType.DMA] * 6 + [
            pltpu.SemaphoreType.DMA((3,)),
            pltpu.SemaphoreType.DMA,
            pltpu.SemaphoreType.DMA((3,)),
        ] + [pltpu.SemaphoreType.DMA] * 4,
        compiler_params=pltpu.CompilerParams(
            collective_id=0, has_side_effects=True, vmem_limit_bytes=48 << 20),
    )(phase, *operands)
    return pl.pallas_call(
        finish,
        name="fock_finish",
        out_shape=jax.ShapeDtypeStruct((1, BT, size, nocc), jnp.float32),
        in_specs=[vmem] * 3,
        out_specs=hbm,
        scratch_shapes=[
            pltpu.VMEM((BT - EARLY, size, nocc), jnp.float32),
            pltpu.SemaphoreType.DMA,
            pltpu.SemaphoreType.DMA((BT - EARLY,)),
        ],
        compiler_params=pltpu.CompilerParams(vmem_limit_bytes=16 << 20),
    )(*parts)


def solution(mesh):
    return jax.shard_map(
        body,
        mesh=mesh,
        in_specs=(P("row", None, None, "col"), P(), P(), P(), P("row", None)),
        out_specs=P("row", None, None, "col"),
        check_vma=False,
    )
```

```python
import jax
import jax.numpy as jnp
from jax import lax
from jax.experimental import pallas as pl
from jax.experimental.pallas import tpu as pltpu
from jax.sharding import PartitionSpec as P

NT = 16
BT = 10
NR = 16
NC = 8
SLOTS = 12
LANES = 128
SPLIT = 8
EARLY = 4
TWO_EARLY = (1, 4, 11, 14)
TWO_LATE = (3, 12)
MESH = pl.DeviceIdType.MESH
S1 = 160
R1 = 96
FRONT = 16
OTHERS = NT - 1
CUTS = (0, 4, 8, 13)
LAST = len(CUTS) - 2


def is_long(m):
    return (m // 4 + m) % 2 == 0


def rows_in(k, long):
    return CUTS[k + 1] - CUTS[k] - int(k == LAST and not long)


def heads_in(k):
    return (CUTS[k + 1] - CUTS[k]) // 2


def rows1(k, long):
    return rows_in(k, long) * SLOTS


def rows2(k, long):
    return rows_in(k, long) * OTHERS + heads_in(k)


def base2(k):
    return sum(-(-rows2(i, True) // 8) * 8 for i in range(k))


P2 = base2(LAST + 1)


def piece_tables():
    halves = range(2)
    pairs = [[], []]
    diagonal = [[], []]
    for h in halves:
        for x in range(BT):
            diagonal[x >= EARLY].append((x, x, h))
            pairs[x >= EARLY] += [(x, y, h) for y in range(x + 1, BT)]
    pieces = []
    for m in range(NR):
        rows = []
        for k, count, size in ((0, 3 if m in TWO_EARLY else 4, SPLIT), (1, 1 if m in TWO_LATE else 2, 13 if is_long(m) else 12)):
            for _ in range(count):
                x, y, h = pairs[k].pop(0)
                rows += [(x, y, h), (y, x, h)]
            while len(rows) < size:
                rows.append(diagonal[k].pop(0))
        pieces.append(rows)
    assert not any(pairs) and not any(diagonal)
    return pieces


def remote(src, dst, send, recv, to):
    return pltpu.make_async_remote_copy(
        src_ref=src, dst_ref=dst, send_sem=send, recv_sem=recv, device_id=to, device_id_type=MESH)


def wait_rows(ref, rows, sem):
    part = ref.at[pl.ds(0, rows)]
    pltpu.make_async_copy(part, part, sem).wait()


def contract(f_ref, dense, columns, out):
    f = f_ref[...]
    for y in columns:
        column = jnp.concatenate([dense[0, y], dense[1, y]], axis=1)
        c_high = column.astype(jnp.bfloat16)
        c_low = (column - c_high.astype(jnp.float32)).astype(jnp.bfloat16)
        stack = jnp.concatenate([c_high, c_low, c_high], axis=0)
        out[y] = jnp.dot(f, stack, preferred_element_type=jnp.float32)


def kernel(
    phase_hbm, blocks_hbm, counts_hbm, amp_hbm, fock_hbm, head_ref, dense, f3_ref,
    phase_ref, blocks_ref, counts_ref, fock_ref, amp, send1, land0, land1, land2, send2, recv2, coef_a, coef_b,
    ftiles, fgather, ffull, early, vtable, table,
    a_sem, p_sem, b_sem, c_sem, f_sem, t_sem, s1_sem, r1_sem, s2_sem, r2_sem, fs_sem, fr_sem, ds_sem, dr_sem,
):
    pieces = piece_tables()
    me = lax.axis_index("row")
    col = lax.axis_index("col")
    long = is_long(me)
    barrier = pltpu.get_barrier_semaphore()
    for d in range(1, NR):
        pl.semaphore_signal(barrier, inc=1, device_id={"row": (me + d) % NR}, device_id_type=MESH)
    for d in range(1, NC):
        pl.semaphore_signal(barrier, inc=1, device_id={"col": (col + d) % NC}, device_id_type=MESH)
    loads = [
        pltpu.make_async_copy(amp_hbm.at[part], amp.at[part], a_sem.at[i])
        for i, part in enumerate((
            (pl.ds(0, EARLY),),
            (pl.ds(EARLY, BT - EARLY), pl.ds(0, EARLY)),
            (pl.ds(EARLY, BT - EARLY), pl.ds(EARLY, BT - EARLY))))
    ]
    for copy in loads:
        copy.start()
    small = [
        pltpu.make_async_copy(phase_hbm, phase_ref, p_sem),
        pltpu.make_async_copy(blocks_hbm, blocks_ref, b_sem),
        pltpu.make_async_copy(counts_hbm, counts_ref, c_sem),
        pltpu.make_async_copy(fock_hbm, fock_ref, f_sem),
    ]
    for copy in small:
        copy.start()

    def pack1(first, last):
        for m in range(NR):
            for j, (x, y, h) in enumerate(pieces[m]):
                if first <= j < last:
                    send1[pl.ds(m * S1 + j * SLOTS, SLOTS), :] = amp[x, y, :, pl.ds(h * LANES, LANES)]

    with jax.named_scope("load"):
        loads[0].wait()
        loads[1].wait()
    with jax.named_scope("pack1_0"):
        pack1(0, SPLIT)
    with jax.named_scope("barrier"):
        pl.semaphore_wait(barrier, NR + NC - 2)

    lands = (land0, land1, land2)

    def send_1(k, to, rows):
        return remote(
            send1.at[pl.ds(to * S1 + CUTS[k] * SLOTS, rows)], lands[k].at[pl.ds(me * R1 + FRONT, rows)],
            s1_sem, r1_sem.at[k], {"row": to})

    def send_2(k, to, rows):
        at = base2(k)
        return remote(
            send2.at[pl.ds(to * P2 + at, rows)], recv2.at[pl.ds(me * P2 + at, rows)],
            s2_sem, r2_sem.at[k], {"row": to})

    def at_size(k, flag, action):
        if k == LAST:
            both(flag, action)
        else:
            action(True)

    def fock_copy(to):
        return remote(ftiles.at[col], fgather.at[col, me], fs_sem, fr_sem, {"row": to})

    def exchange(d):
        return remote(fgather.at[col], fgather.at[col], ds_sem, dr_sem, {"col": (col + d) % NC})

    def both(flag, action):
        for value in (True, False):
            @pl.when(flag == value)
            def _():
                action(value)

    def start1(k):
        @pl.loop(1, NR)
        def _(d):
            to = (me + d) % NR
            at_size(k, is_long(to), lambda value: send_1(k, to, rows1(k, value)).start())

    with jax.named_scope("start1"):
        for k in range(LAST):
            start1(k)

    with jax.named_scope("pack1_1"):
        loads[2].wait()
        pack1(SPLIT, 13)

    with jax.named_scope("start1b"):
        start1(LAST)

    for copy in small:
        copy.wait()
    for q in range(5):
        ftiles[q] = fock_ref[2 * q:2 * q + 2, :LANES]
    for q in range(5):
        ftiles[5 + q % 3, :, pl.ds(q // 3 * 32, 32)] = fock_ref[2 * q:2 * q + 2, LANES:]

    @pl.loop(1, NR)
    def _(d):
        fock_copy((me + d) % NR).start()

    with jax.named_scope("tables"):
        for k in range(LAST + 1):
            rows = rows1(k, True)
            lands[k][pl.ds(me * R1 + FRONT, rows), :] = send1[pl.ds(me * S1 + CUTS[k] * SLOTS, rows), :]
        fgather[col, me] = ftiles[col]
        row = lax.broadcasted_iota(jnp.int32, (16, LANES), 0)
        two_early = (me == 1) | (me == 4) | (me == 11) | (me == 14)
        two_late = (me == 3) | (me == 12)
        is_pair = (row < 12) & ~((row // 2 == 3) & two_early) & ~((row // 2 == 5) & two_late)
        one = jnp.ones((16, LANES), jnp.float32)
        coef_a[0] = one
        coef_b[0] = jnp.zeros((16, LANES), jnp.float32)
        coef_a[1] = jnp.where(is_pair, 0.0, -one)
        coef_b[1] = jnp.where(is_pair, -one, 0.0)
        up_mask = (row % 2 == 0) & (row < 12)

        sub = lax.broadcasted_iota(jnp.int32, (8, LANES), 0)
        lane = lax.broadcasted_iota(jnp.int32, (8, LANES), 1)
        mine = ((sub % 2) * 8 + lane // NT - phase_ref[0, 0] + NR) % NR
        other = (mine + lane) % NT
        low = jnp.minimum(mine, other)
        high = jnp.maximum(mine, other)
        ident = low * NT - (low * (low - 1)) // 2 + (high - low)

        def look(d, at):
            for slot in range(SLOTS):
                block = jnp.where(slot < counts_ref[d], blocks_ref[d, slot], -1)
                at = jnp.where(ident == block, d * R1 + (FRONT + slot), at)
            return at

        at = lax.fori_loop(0, NR, look, jnp.full((8, LANES), FRONT, jnp.int32))
        vtable[...] = jnp.where(sub < 2, at, jnp.where(other > mine, 1, 0))
        to_smem = pltpu.make_async_copy(vtable, table, t_sem)
        to_smem.start()
        to_smem.wait()

    def pack2(k, to, dst, slot):
        first = CUTS[k]
        n = CUTS[k + 1] - first
        base = slot * P2 + base2(k)
        land = lands[k]
        for c in range(NT):
            at = table[to // 8, (to % 8) * NT + c]
            if c == 0:
                dst[pl.ds(base, heads_in(k)), :] = land[pl.ds(at, heads_in(k), stride=2 * SLOTS), :]
                continue
            kind = table[2 + to // 8, (to % 8) * NT + c]
            v = land[pl.ds(at, n, stride=SLOTS), :]
            up = land[pl.ds(at + SLOTS, n, stride=SLOTS), :]
            down = land[pl.ds(at - SLOTS, n, stride=SLOTS), :]
            swapped = jnp.where(up_mask[first:first + n], up, down)
            dst[pl.ds(base + heads_in(k) + c - 1, n, stride=OTHERS), :] = (
                coef_a[kind, first:first + n] * v + coef_b[kind, first:first + n] * swapped)

    for k in range(LAST + 1):
        with jax.named_scope(f"wait1_{k}"):
            at_size(k, long, lambda value: wait_rows(lands[k], OTHERS * rows1(k, value), r1_sem.at[k]))

        with jax.named_scope(f"pack2_{k}"):
            @pl.loop(1, NR)
            def _(d):
                to = (me + d) % NR
                pack2(k, to, send2, to)
                at_size(k, long, lambda value: send_2(k, to, rows2(k, value)).start())

            pack2(k, me, recv2, me)

    with jax.named_scope("waitf"):
        wait_rows(send1, OTHERS * 2, fr_sem)
        for d in range(1, NC):
            exchange(d).start()
        both(long, lambda value: wait_rows(
            send1,
            OTHERS * CUTS[LAST] * SLOTS + (8 - value) * rows1(LAST, True) + (7 + value) * rows1(LAST, False),
            s1_sem))

    def put(h, y, at, rows):
        target, column = (early, y) if y < EARLY else (dense, y - EARLY)
        target[h, column, at, :] = rows

    def assemble(k):
        for m in range(NR):
            for j, (x, y, h) in enumerate(pieces[m]):
                if not CUTS[k] <= j < CUTS[k + 1]:
                    continue
                i = j - CUTS[k]
                base = m * P2 + base2(k)
                rows = recv2[pl.ds(base + heads_in(k) + i * OTHERS, OTHERS), :]
                put(h, y, pl.ds(x + BT, OTHERS, stride=BT), rows)
                if x < y:
                    head = recv2[pl.ds(base + i // 2, 1), :]
                    put(h, y, pl.ds(x, 1), head)
                    put(h, x, pl.ds(y, 1), -head)
                elif x == y:
                    put(h, y, pl.ds(x, 1), jnp.zeros((1, LANES), jnp.float32))

    for k in range(LAST):
        with jax.named_scope(f"wait2_{k}"):
            wait_rows(recv2, OTHERS * rows2(k, True), r2_sem.at[k])

        with jax.named_scope(f"assemble_{k}"):
            assemble(k)

    with jax.named_scope("fock"):
        wait_rows(send1, (NC - 1) * 2 * NR, dr_sem)
        wait_rows(send1, (NC - 1) * 2 * NR, ds_sem)
        wait_rows(send1, OTHERS * 2, fs_sem)
        for d in range(NR):
            for q in range(5):
                at = pl.ds(d * BT + 2 * q, 2)
                ffull[at, :LANES] = fgather[q, d]
                ffull[at, LANES:] = fgather[5 + q % 3, d, :, pl.ds(q // 3 * 32, 32)]
        turn = (me - phase_ref[0, 0] + NR) % NR * BT
        size = NT * BT
        wide = lax.broadcasted_iota(jnp.int32, (size, 3 * size), 1)
        part = (wide >= size).astype(jnp.int32) + (wide >= 2 * size).astype(jnp.int32)
        shifted = wide - part * size + turn
        shifted = jnp.where(shifted >= size, shifted - size, shifted)
        picks = (lax.broadcasted_iota(jnp.int32, (size, 3 * size), 0) == shifted).astype(jnp.float32)
        f = ffull[...]
        f_high = f.astype(jnp.bfloat16)
        f_low = (f - f_high.astype(jnp.float32)).astype(jnp.bfloat16)
        f3_ref[...] = (
            jnp.dot(f_high, jnp.where(part < 2, picks, 0.0).astype(jnp.bfloat16), preferred_element_type=jnp.float32)
            + jnp.dot(f_low, jnp.where(part == 2, picks, 0.0).astype(jnp.bfloat16), preferred_element_type=jnp.float32)
        ).astype(jnp.bfloat16)

    with jax.named_scope("matmul_0"):
        contract(f3_ref, early, range(EARLY), head_ref)

    with jax.named_scope(f"wait2_{LAST}"):
        both(long, lambda value: wait_rows(
            recv2, (8 - value) * rows2(LAST, True) + (7 + value) * rows2(LAST, False), r2_sem.at[LAST]))

    with jax.named_scope(f"assemble_{LAST}"):
        assemble(LAST)

    with jax.named_scope("drain"):
        both(long, lambda value: wait_rows(send2, OTHERS * sum(rows2(k, value) for k in range(LAST + 1)), s2_sem))


def finish(head_ref, dense, f3_ref, out_hbm, late, h_sem, o_sem):
    copies = [pltpu.make_async_copy(head_ref, out_hbm.at[0, pl.ds(0, EARLY)], h_sem)]
    copies[0].start()
    for y in range(BT - EARLY):
        contract(f3_ref, dense, (y,), late)
        copies.append(pltpu.make_async_copy(late.at[y], out_hbm.at[0, EARLY + y], o_sem.at[y]))
        copies[-1].start()
    for copy in copies:
        copy.wait()


def body(amplitudes, old_blocks, old_counts, new_phase, fock):
    nocc = amplitudes.shape[3]
    turned = jnp.transpose(amplitudes, (1, 2, 0, 3))
    phase = new_phase.reshape(1, 1)
    hbm = pl.BlockSpec(memory_space=pltpu.HBM)
    operands = [
        pltpu.with_memory_space_constraint(array, pltpu.HBM)
        for array in (old_blocks, old_counts, turned, fock)
    ]
    size = NT * BT
    vmem = pl.BlockSpec(memory_space=pltpu.VMEM)
    parts = pl.pallas_call(
        kernel,
        name="fock_two_phase",
        out_shape=(
            jax.ShapeDtypeStruct((EARLY, size, nocc), jnp.float32),
            jax.ShapeDtypeStruct((2, BT - EARLY, size, LANES), jnp.float32),
            jax.ShapeDtypeStruct((size, 3 * size), jnp.bfloat16),
        ),
        in_specs=[pl.BlockSpec(memory_space=pl.ANY)] + [hbm] * 4,
        out_specs=(vmem,) * 3,
        scratch_shapes=[
            pltpu.SMEM(phase.shape, jnp.int32),
            pltpu.SMEM(old_blocks.shape, jnp.int32),
            pltpu.SMEM(old_counts.shape, jnp.int32),
            pltpu.VMEM(fock.shape, jnp.float32),
            pltpu.VMEM(turned.shape, jnp.float32),
            pltpu.VMEM((NR * S1, LANES), jnp.float32),
            pltpu.VMEM((NR * R1, LANES), jnp.float32),
            pltpu.VMEM((NR * R1, LANES), jnp.float32),
            pltpu.VMEM((NR * R1, LANES), jnp.float32),
            pltpu.VMEM((NR * P2, LANES), jnp.float32),
            pltpu.VMEM((NR * P2, LANES), jnp.float32),
            pltpu.VMEM((2, 16, LANES), jnp.float32),
            pltpu.VMEM((2, 16, LANES), jnp.float32),
            pltpu.VMEM((NC, 2, LANES), jnp.float32),
            pltpu.VMEM((NC, NR, 2, LANES), jnp.float32),
            pltpu.VMEM((size, size), jnp.float32),
            pltpu.VMEM((2, EARLY, size, LANES), jnp.float32),
            pltpu.VMEM((8, LANES), jnp.int32),
            pltpu.SMEM((8, LANES), jnp.int32),
        ] + [pltpu.SemaphoreType.DMA((3,))] + [pltpu.SemaphoreType.DMA] * 6 + [
            pltpu.SemaphoreType.DMA((3,)),
            pltpu.SemaphoreType.DMA,
            pltpu.SemaphoreType.DMA((3,)),
        ] + [pltpu.SemaphoreType.DMA] * 4,
        compiler_params=pltpu.CompilerParams(
            collective_id=0, has_side_effects=True, vmem_limit_bytes=48 << 20),
    )(phase, *operands)
    return pl.pallas_call(
        finish,
        name="fock_finish",
        out_shape=jax.ShapeDtypeStruct((1, BT, size, nocc), jnp.float32),
        in_specs=[vmem] * 3,
        out_specs=hbm,
        scratch_shapes=[
            pltpu.VMEM((BT - EARLY, size, nocc), jnp.float32),
            pltpu.SemaphoreType.DMA,
            pltpu.SemaphoreType.DMA((BT - EARLY,)),
        ],
        compiler_params=pltpu.CompilerParams(vmem_limit_bytes=16 << 20),
    )(*parts)


def solution(mesh):
    return jax.shard_map(
        body,
        mesh=mesh,
        in_specs=(P("row", None, None, "col"), P(), P(), P(), P("row", None)),
        out_specs=P("row", None, None, "col"),
        check_vma=False,
    )
```
